16 devices in a mesh: dp: 2 (over y, z), sp: 8 (over x, core).
Axes of the slice: x: 4, y: 2, z: 1, core: 2. Of those that a mesh axis runs over, the one named last changes fastest.
The devices are a block of a 4x4x8 slice.
Arguments:
- hidden: bfloat16 [32, 128, 2560], P('dp', 'sp'), parts along dimension 0
- attn_norm: bfloat16 [2560], replicated
- w_q: bfloat16 [2560, 32, 128], replicated
- w_k: bfloat16 [2560, 8, 128], replicated
- w_v: bfloat16 [2560, 8, 128], replicated
- w_o: bfloat16 [32, 128, 2560], replicated
- mlp_norm: bfloat16 [2560], replicated
- w_gate: bfloat16 [2560, 9728], replicated
- w_up: bfloat16 [2560, 9728], replicated
- w_down: bfloat16 [9728, 2560], replicated
- mamba_norm: bfloat16 [2560], replicated
- w_in_x: bfloat16 [2560, 5120], replicated
- w_in_z: bfloat16 [2560, 5120], replicated
- conv_w: bfloat16 [4, 5120], replicated
- conv_b: bfloat16 [5120], replicated
- w_xproj: bfloat16 [5120, 192], replicated
- dt_norm: float32 [160], replicated
- b_norm: float32 [16], replicated
- c_norm: float32 [16], replicated
- w_dt: bfloat16 [160, 5120], replicated
- dt_bias: float32 [5120], replicated
- a_log: float32 [5120, 16], replicated
- d_skip: float32 [5120], replicated
- w_out: bfloat16 [5120, 2560], replicated
Outputs:
- output: bfloat16 [32, 128, 2560], P('dp', 'sp'), parts along dimension 0
There are 2 independent parts. The reference program is written for one: setup_inputs(seed, part) draws one part's arguments, and reference() takes and returns one part's arrays. A program takes and returns all parts, laid end to end along the dimension named above; an argument that names none is the same for every part.
All inputs are finite; a program needn't handle non-finite values.
Results may differ from the reference program's by a relative error of at most 0.02.
Values are sent between devices in bfloat16 or wider.
A program may use at most 768 MiB of HBM per device.

```python
import jax
import jax.numpy as jnp
from jax import lax

BATCH = 16
TOK_DEV = 16
SEQ = 128
D = 2560
HEADS = 32
KV_HEADS = 8
HEAD = 128
FF = 9728
INNER = 5120
STATE = 16
DT_RANK = 160
CONV = 4
EPS = 1e-6


def setup_inputs(seed: int = 0, part: int = 0) -> dict:
    key_list = jax.random.split(jax.random.key(seed), 24)
    part_key = jax.random.fold_in(key_list[0], part)

    def normal(key_idx, arr_shape, std_dev):
        return jax.random.normal(key_list[key_idx], arr_shape, jnp.float32) * std_dev

    def uniform(key_idx, arr_shape, lower_b, upper_b):
        return jax.random.uniform(key_list[key_idx], arr_shape, jnp.float32, lower_b, upper_b)

    qk_scale = 1.5 * D ** -0.5
    return {
        "hidden": jax.random.normal(part_key, (BATCH, SEQ, D), jnp.float32).astype(jnp.bfloat16),
        "attn_norm": uniform(1, (D,), 0.5, 1.5).astype(jnp.bfloat16),
        "w_q": normal(2, (D, HEADS, HEAD), qk_scale).astype(jnp.bfloat16),
        "w_k": normal(3, (D, KV_HEADS, HEAD), qk_scale).astype(jnp.bfloat16),
        "w_v": normal(4, (D, KV_HEADS, HEAD), D ** -0.5).astype(jnp.bfloat16),
        "w_o": normal(5, (HEADS, HEAD, D), (HEADS * HEAD) ** -0.5).astype(jnp.bfloat16),
        "mlp_norm": uniform(6, (D,), 0.5, 1.5).astype(jnp.bfloat16),
        "w_gate": normal(7, (D, FF), D ** -0.5).astype(jnp.bfloat16),
        "w_up": normal(8, (D, FF), D ** -0.5).astype(jnp.bfloat16),
        "w_down": normal(9, (FF, D), FF ** -0.5).astype(jnp.bfloat16),
        "mamba_norm": uniform(10, (D,), 0.5, 1.5).astype(jnp.bfloat16),
        "w_in_x": normal(11, (D, INNER), D ** -0.5).astype(jnp.bfloat16),
        "w_in_z": normal(12, (D, INNER), D ** -0.5).astype(jnp.bfloat16),
        "conv_w": normal(13, (CONV, INNER), 0.5).astype(jnp.bfloat16),
        "conv_b": normal(14, (INNER,), 0.3).astype(jnp.bfloat16),
        "w_xproj": normal(15, (INNER, DT_RANK + 2 * STATE), INNER ** -0.5).astype(jnp.bfloat16),
        "dt_norm": uniform(16, (DT_RANK,), 0.5, 1.5),
        "b_norm": uniform(17, (STATE,), 0.5, 1.5) * TOK_DEV ** 0.5,
        "c_norm": uniform(18, (STATE,), 0.5, 1.5),
        "w_dt": normal(19, (DT_RANK, INNER), DT_RANK ** -0.5).astype(jnp.bfloat16),
        "dt_bias": jnp.log(uniform(20, (INNER,), 0.25, 1.0) / TOK_DEV),
        "a_log": jnp.log(uniform(21, (INNER, STATE), 0.3, 1.5)),
        "d_skip": uniform(22, (INNER,), -1.5, 1.5),
        "w_out": normal(23, (INNER, D), INNER ** -0.5).astype(jnp.bfloat16),
    }


def rms_scale(values, gain_vec):
    values_f = values.astype(jnp.float32)
    inv_rms = lax.rsqrt(jnp.mean(values_f * values_f, axis=-1, keepdims=True) + EPS)
    return values_f * inv_rms * gain_vec.astype(jnp.float32)


def attention_layer(hidden, attn_norm, w_q, w_k, w_v, w_o):
    n_batch, seq_len, model_dim = hidden.shape
    groups = HEADS // KV_HEADS
    normed = rms_scale(hidden, attn_norm).astype(jnp.bfloat16).reshape(n_batch * seq_len, model_dim)
    queries = jnp.dot(normed, w_q.reshape(model_dim, HEADS * HEAD), preferred_element_type=jnp.float32).astype(jnp.bfloat16)
    key_proj = jnp.dot(normed, w_k.reshape(model_dim, KV_HEADS * HEAD), preferred_element_type=jnp.float32).astype(jnp.bfloat16)
    val_proj = jnp.dot(normed, w_v.reshape(model_dim, KV_HEADS * HEAD), preferred_element_type=jnp.float32).astype(jnp.bfloat16)
    queries = queries.reshape(n_batch, seq_len, KV_HEADS, groups, HEAD).transpose(2, 0, 1, 3, 4)
    key_proj = key_proj.reshape(n_batch, seq_len, KV_HEADS, HEAD).transpose(2, 0, 1, 3)
    val_proj = val_proj.reshape(n_batch, seq_len, KV_HEADS, HEAD).transpose(2, 0, 1, 3)
    causal = jnp.arange(seq_len)[:, None] >= jnp.arange(seq_len)[None, :]

    def one_group(operands):
        q_grp, k_grp, v_grp = operands
        scores = jnp.einsum("bqgd,bsd->bgqs", q_grp.astype(jnp.float32), k_grp.astype(jnp.float32)) * HEAD ** -0.5
        scores = jnp.where(causal, scores, -jnp.inf)
        attn_prob = jax.nn.softmax(scores, axis=-1).astype(jnp.bfloat16)
        return jnp.einsum("bgqs,bsd->bqgd", attn_prob.astype(jnp.float32), v_grp.astype(jnp.float32)).astype(jnp.bfloat16)

    attn_out = lax.map(one_group, (queries, key_proj, val_proj))
    attn_out = attn_out.transpose(1, 2, 0, 3, 4).reshape(n_batch * seq_len, HEADS * HEAD)
    proj_out = jnp.dot(attn_out, w_o.reshape(HEADS * HEAD, model_dim), preferred_element_type=jnp.float32)
    return (hidden.astype(jnp.float32) + proj_out.reshape(n_batch, seq_len, model_dim)).astype(jnp.bfloat16)


def mlp_layer(hidden, mlp_norm, w_gate, w_up, w_down):
    model_dim = hidden.shape[-1]
    normed = rms_scale(hidden, mlp_norm).astype(jnp.bfloat16).reshape(-1, model_dim)
    gate_pre = jnp.dot(normed, w_gate, preferred_element_type=jnp.float32)
    up_proj = jnp.dot(normed, w_up, preferred_element_type=jnp.float32)
    act_val = (jax.nn.silu(gate_pre) * up_proj).astype(jnp.bfloat16)
    down_out = jnp.dot(act_val, w_down, preferred_element_type=jnp.float32)
    return (hidden.astype(jnp.float32) + down_out.reshape(hidden.shape)).astype(jnp.bfloat16)


def mamba_mixer(hidden, mamba_norm, w_in_x, w_in_z, conv_w, conv_b, w_xproj, dt_norm, b_norm, c_norm, w_dt, dt_bias, a_log, d_skip, w_out):
    n_batch, seq_len, model_dim = hidden.shape
    normed = rms_scale(hidden, mamba_norm).astype(jnp.bfloat16).astype(jnp.float32)
    x_inner = jnp.einsum("btd,de->tbe", normed, w_in_x.astype(jnp.float32)).astype(jnp.bfloat16)
    z_gate = jnp.einsum("btd,de->tbe", normed, w_in_z.astype(jnp.float32)).astype(jnp.bfloat16)
    padded = jnp.concatenate([jnp.zeros((CONV - 1, n_batch, INNER), jnp.bfloat16), x_inner], axis=0)
    conv_acc = conv_b.astype(jnp.float32)
    for tap_idx in range(CONV):
        conv_acc = conv_acc + padded[tap_idx:tap_idx + seq_len].astype(jnp.float32) * conv_w[tap_idx].astype(jnp.float32)
    x_conv = jax.nn.silu(conv_acc).astype(jnp.bfloat16)
    x_dbl = jnp.einsum("tbe,er->tbr", x_conv.astype(jnp.float32), w_xproj.astype(jnp.float32))
    dt_in = rms_scale(x_dbl[..., :DT_RANK], dt_norm).astype(jnp.bfloat16)
    b_mat = rms_scale(x_dbl[..., DT_RANK:DT_RANK + STATE], b_norm)
    c_mat = rms_scale(x_dbl[..., DT_RANK + STATE:], c_norm)
    step_size = jax.nn.softplus(jnp.einsum("tbr,re->tbe", dt_in.astype(jnp.float32), w_dt.astype(jnp.float32)) + dt_bias)
    a_mat = -jnp.exp(a_log)

    def scan_step(ssm_state, inputs):
        step_t, x_t, b_t, c_t = inputs
        decay_t = jnp.exp(step_t[:, :, None] * a_mat)
        ssm_state = decay_t * ssm_state + (step_t * x_t.astype(jnp.float32))[:, :, None] * b_t[:, None, :]
        return ssm_state, jnp.sum(ssm_state * c_t[:, None, :], axis=-1)

    zero_state = jnp.zeros((n_batch, INNER, STATE), jnp.float32)
    y_seq = lax.scan(scan_step, zero_state, (step_size, x_conv, b_mat, c_mat))[1]
    gated_y = ((y_seq + d_skip * x_conv.astype(jnp.float32)) * jax.nn.silu(z_gate.astype(jnp.float32))).astype(jnp.bfloat16)
    mamba_out = jnp.einsum("tbe,ed->btd", gated_y.astype(jnp.float32), w_out.astype(jnp.float32))
    return (hidden.astype(jnp.float32) + mamba_out).astype(jnp.bfloat16)


def reference(hidden, attn_norm, w_q, w_k, w_v, w_o, mlp_norm, w_gate, w_up, w_down, mamba_norm, w_in_x, w_in_z, conv_w, conv_b, w_xproj, dt_norm, b_norm, c_norm, w_dt, dt_bias, a_log, d_skip, w_out):
    after_attn = attention_layer(hidden, attn_norm, w_q, w_k, w_v, w_o)
    after_mlp = mlp_layer(after_attn, mlp_norm, w_gate, w_up, w_down)
    return mamba_mixer(after_mlp, mamba_norm, w_in_x, w_in_z, conv_w, conv_b, w_xproj, dt_norm, b_norm, c_norm, w_dt, dt_bias, a_log, d_skip, w_out)
```

```python
import functools
import math

import jax
import jax.numpy as jnp
from jax import lax
from jax.experimental import pallas as pl
from jax.experimental.pallas import tpu as pltpu
from jax.sharding import PartitionSpec as P

EPS = 1e-6
CONV = 4
F32 = jnp.float32
BF16 = jnp.bfloat16
LOG2E = 1.0 / math.log(2.0)


def dot(a, b):
    return jnp.dot(a, b, preferred_element_type=F32)


def dot_nt(a, b):
    return lax.dot_general(a, b, (((1,), (1,)), ((), ())), preferred_element_type=F32)


def rms_rows(v, gain):
    v = v.astype(F32)
    inv = lax.rsqrt(jnp.mean(v * v, axis=-1, keepdims=True) + EPS)
    return v * inv * gain.astype(F32)


def silu(v):
    return v / (1.0 + jnp.exp(-v))


def softplus(v):
    return jnp.maximum(v, 0.0) + jnp.log1p(jnp.exp(-jnp.abs(v)))


def full(shape):
    nd = len(shape)
    return pl.BlockSpec(shape, lambda i: (0,) * nd, pipeline_mode=pl.Buffered(1))


def params(limit=60 << 20):
    return pltpu.CompilerParams(dimension_semantics=("arbitrary",), vmem_limit_bytes=limit)


def attn_kernel(nq, nkv, seq, hd, x_ref, g_ref, wq_ref, wk_ref, wv_ref, wo_ref, h_ref,
                a_s, q_s, kv_s, acc_s):
    i = pl.program_id(0)
    rows, tile = q_s.shape[1], q_s.shape[2]
    grp = tile // hd
    nb = rows // seq
    n1 = nq + 2 * nkv

    @pl.when(i == 0)
    def _():
        a_s[...] = rms_rows(x_ref[...], g_ref[...]).astype(BF16)
        acc_s[...] = x_ref[...].astype(F32)

    @pl.when(i < nq)
    def _():
        q_s[jnp.minimum(i, nq - 1)] = dot(a_s[...], wq_ref[...]).astype(BF16)

    def put_kv(w_ref):
        val = dot(a_s[...], w_ref[...]).astype(BF16)
        base = (i - nq) * grp
        for h in range(grp):
            kv_s[base + h] = val[:, h * hd:(h + 1) * hd]

    @pl.when((i >= nq) & (i < nq + nkv))
    def _():
        put_kv(wk_ref)

    @pl.when((i >= nq + nkv) & (i < n1))
    def _():
        put_kv(wv_ref)

    @pl.when(i >= n1)
    def _():
        j = i - n1
        outs = []
        row_t = lax.broadcasted_iota(jnp.int32, (grp * seq, seq), 0) % seq
        col_t = lax.broadcasted_iota(jnp.int32, (grp * seq, seq), 1)
        causal = row_t >= col_t
        for b in range(nb):
            qb = q_s[j, b * seq:(b + 1) * seq, :]
            q4 = jnp.concatenate([qb[:, g * hd:(g + 1) * hd] for g in range(grp)], axis=0)
            kb = kv_s[j, b * seq:(b + 1) * seq, :]
            vb = kv_s[nkv * grp + j, b * seq:(b + 1) * seq, :]
            s = dot_nt(q4, kb) * (hd ** -0.5)
            s = jnp.where(causal, s, -jnp.inf)
            e = jnp.exp(s - jnp.max(s, axis=-1, keepdims=True))
            p = (e / jnp.sum(e, axis=-1, keepdims=True)).astype(BF16)
            o = dot(p, vb).astype(BF16)
            outs.append(jnp.concatenate([o[g * seq:(g + 1) * seq, :] for g in range(grp)], axis=1))
        o_all = jnp.concatenate(outs, axis=0)
        acc_s[...] += dot(o_all, wo_ref[...])

    @pl.when(i == pl.num_programs(0) - 1)
    def _():
        h_ref[...] = acc_s[...].astype(BF16)


def attention(x, g, wq, wk, wv, wo, seq, hd):
    rows, dm = x.shape
    tile = (wq.shape[1] // wk.shape[1]) * hd
    nq, nkv = wq.shape[1] // tile, wk.shape[1] // tile
    no = wo.shape[0] // tile
    n1 = nq + 2 * nkv
    return pl.pallas_call(
        functools.partial(attn_kernel, nq, nkv, seq, hd),
        grid=(n1 + no,),
        out_shape=jax.ShapeDtypeStruct((rows, dm), BF16),
        in_specs=[
            full((rows, dm)), full((1, dm)),
            pl.BlockSpec((dm, tile), lambda i: (0, jnp.clip(i, 0, nq - 1))),
            pl.BlockSpec((dm, tile), lambda i: (0, jnp.clip(i - nq, 0, nkv - 1))),
            pl.BlockSpec((dm, tile), lambda i: (0, jnp.clip(i - nq - nkv, 0, nkv - 1))),
            pl.BlockSpec((tile, dm), lambda i: (jnp.clip(i - n1, 0, no - 1), 0)),
        ],
        out_specs=full((rows, dm)),
        scratch_shapes=[
            pltpu.VMEM((rows, dm), BF16),
            pltpu.VMEM((nq, rows, tile), BF16),
            pltpu.VMEM((2 * nkv * (tile // hd), rows, hd), BF16),
            pltpu.VMEM((rows, dm), F32),
        ],
        compiler_params=params(),
        name="attention",
    )(x, g, wq, wk, wv, wo)


def mlp_kernel(h_ref, g_ref, wg_ref, wu_ref, wd_ref, o_ref, m_s, act_s, acc_s):
    i = pl.program_id(0)
    n = pl.num_programs(0) - 1

    @pl.when(i == 0)
    def _():
        m_s[...] = rms_rows(h_ref[...], g_ref[...]).astype(BF16)
        acc_s[...] = h_ref[...].astype(F32)
        gate = dot(m_s[...], wg_ref[...])
        up = dot(m_s[...], wu_ref[...])
        act_s[0] = (silu(gate) * up).astype(BF16)

    @pl.when((i > 0) & (i < n))
    def _():
        gate = dot(m_s[...], wg_ref[...])
        up = dot(m_s[...], wu_ref[...])
        acc_s[...] += dot(act_s[lax.rem(i + 1, 2)], wd_ref[...])
        act_s[lax.rem(i, 2)] = (silu(gate) * up).astype(BF16)

    @pl.when(i == n)
    def _():
        o_ref[...] = (acc_s[...] + dot(act_s[lax.rem(i + 1, 2)], wd_ref[...])).astype(BF16)


def mlp(h, g, wg, wu, wd, tile=512):
    rows, dm = h.shape
    n = wg.shape[1] // tile
    return pl.pallas_call(
        mlp_kernel,
        grid=(n + 1,),
        out_shape=jax.ShapeDtypeStruct((rows, dm), BF16),
        in_specs=[
            full((rows, dm)), full((1, dm)),
            pl.BlockSpec((dm, tile), lambda i: (0, jnp.minimum(i, n - 1))),
            pl.BlockSpec((dm, tile), lambda i: (0, jnp.minimum(i, n - 1))),
            pl.BlockSpec((tile, dm), lambda i: (jnp.maximum(i - 1, 0), 0)),
        ],
        out_specs=full((rows, dm)),
        scratch_shapes=[
            pltpu.VMEM((rows, dm), BF16),
            pltpu.VMEM((2, rows, tile), BF16),
            pltpu.VMEM((rows, dm), F32),
        ],
        compiler_params=params(),
        name="mlp",
    )(h, g, wg, wu, wd)


def mamba_kernel(ne, seq, dt_rank, n_state, h_ref, g_ref, wx_ref, cw_ref, cb_ref, wxp_ref,
                 dtn_ref, bn_ref, cn_ref, wdt_ref, dtb_ref, alog_ref, dsk_ref, wz_ref, wo_ref, o_ref,
                 u_s, c_s, r_s, dt_s, b_s, cc_s, d_s, x_s, y_s, a_s, gate_s, acc_s):
    i = pl.program_id(0)
    rows, dm = u_s.shape
    tile = c_s.shape[2]
    sub = tile // 128
    nb = rows // seq

    @pl.when(i == 0)
    def _():
        u_s[...] = rms_rows(h_ref[...], g_ref[...]).astype(BF16)
        acc_s[...] = h_ref[...].astype(F32)
        r_s[...] = jnp.zeros_like(r_s)

    @pl.when(i < ne)
    def _():
        xi = dot(u_s[...], wx_ref[...]).astype(BF16).astype(F32)
        t_idx = lax.broadcasted_iota(jnp.int32, xi.shape, 0) % seq
        acc = cb_ref[...].astype(F32) + xi * cw_ref[CONV - 1:CONV, :].astype(F32)
        for s in range(1, CONV):
            prev = jnp.where(t_idx >= s, pltpu.roll(xi, s, 0), 0.0)
            acc = acc + prev * cw_ref[CONV - 1 - s:CONV - s, :].astype(F32)
        c = silu(acc).astype(BF16)
        c_s[jnp.minimum(i, ne - 1)] = c
        r_s[...] += dot_nt(c, wxp_ref[...])

    @pl.when(i == ne)
    def _():
        r = r_s[...]
        dt_s[...] = rms_rows(r[:, :dt_rank], dtn_ref[...]).astype(BF16)
        bm = rms_rows(r[:, dt_rank:dt_rank + n_state], bn_ref[...])
        cm = rms_rows(r[:, dt_rank + n_state:], cn_ref[...])
        for n in range(n_state):
            b_s[n] = jnp.broadcast_to(bm[:, n:n + 1], (rows, 128))
            cc_s[n] = jnp.broadcast_to(cm[:, n:n + 1], (rows, 128))

    @pl.when(i >= ne)
    def _():
        e = i - ne
        delta = softplus(dot(dt_s[...], wdt_ref[...]) + dtb_ref[...])
        dx = delta * c_s[e].astype(F32)
        a2 = -jnp.exp(alog_ref[...]) * LOG2E
        for j in range(sub):
            d_s[pl.ds(j, rows, stride=sub), :] = delta[:, j * 128:(j + 1) * 128]
            x_s[pl.ds(j, rows, stride=sub), :] = dx[:, j * 128:(j + 1) * 128]
            a_s[pl.ds(j, n_state, stride=sub), :] = a2[:, j * 128:(j + 1) * 128]

        def step(t, state):
            new = []
            for b in range(nb):
                tok = b * seq + t
                row = pl.multiple_of(tok * sub, sub)
                dl = d_s[pl.ds(row, sub), :]
                dxt = x_s[pl.ds(row, sub), :]
                parts = [None] * 4
                for n in range(n_state):
                    bb = b_s[n, pl.ds(tok, sub, stride=0), :]
                    ct = cc_s[n, pl.ds(tok, sub, stride=0), :]
                    s = jnp.exp2(dl * a_s[n * sub:(n + 1) * sub, :]) * state[b * n_state + n] + dxt * bb
                    new.append(s)
                    term = s * ct
                    parts[n % 4] = term if parts[n % 4] is None else parts[n % 4] + term
                y_s[pl.ds(row, sub), :] = (parts[0] + parts[1]) + (parts[2] + parts[3])
            return tuple(new)

        zero = jnp.zeros((sub, 128), F32)
        lax.fori_loop(0, seq, step, (zero,) * (nb * n_state), unroll=2)
        z = dot(u_s[...], wz_ref[...]).astype(BF16).astype(F32)
        for j in range(sub):
            lanes = slice(j * 128, (j + 1) * 128)
            y = y_s[pl.ds(j, rows, stride=sub), :] + dsk_ref[:, lanes] * c_s[e, :, lanes].astype(F32)
            gate_s[:, lanes] = (y * silu(z[:, lanes])).astype(BF16)
        acc_s[...] += dot(gate_s[...], wo_ref[...])

    @pl.when(i == pl.num_programs(0) - 1)
    def _():
        o_ref[...] = acc_s[...].astype(BF16)


def mamba(h, g, wx, wz, cw, cb, wxp_t, dtn, bn, cn, wdt, dtb, alog_t, dsk, wo, seq, tile=1024):
    rows, dm = h.shape
    inner = wx.shape[1]
    dt_rank, n_state = wdt.shape[0], alog_t.shape[0]
    nr = wxp_t.shape[0]
    ne = inner // tile
    sub = tile // 128
    pa = lambda i: (0, jnp.minimum(i, ne - 1))
    pb = lambda i: (0, jnp.maximum(i - ne, 0))
    return pl.pallas_call(
        functools.partial(mamba_kernel, ne, seq, dt_rank, n_state),
        grid=(2 * ne,),
        out_shape=jax.ShapeDtypeStruct((rows, dm), BF16),
        in_specs=[
            full((rows, dm)), full((1, dm)),
            pl.BlockSpec((dm, tile), pa),
            pl.BlockSpec((CONV, tile), pa),
            pl.BlockSpec((1, tile), pa),
            pl.BlockSpec((nr, tile), pa),
            full((1, dt_rank)), full((1, n_state)), full((1, n_state)),
            pl.BlockSpec((dt_rank, tile), pb),
            pl.BlockSpec((1, tile), pb),
            pl.BlockSpec((n_state, tile), pb),
            pl.BlockSpec((1, tile), pb),
            pl.BlockSpec((dm, tile), pb),
            pl.BlockSpec((tile, dm), lambda i: (jnp.maximum(i - ne, 0), 0)),
        ],
        out_specs=full((rows, dm)),
        scratch_shapes=[
            pltpu.VMEM((rows, dm), BF16),
            pltpu.VMEM((ne, rows, tile), BF16),
            pltpu.VMEM((rows, nr), F32),
            pltpu.VMEM((rows, dt_rank), BF16),
            pltpu.VMEM((n_state, rows, 128), F32),
            pltpu.VMEM((n_state, rows, 128), F32),
            pltpu.VMEM((rows * sub, 128), F32),
            pltpu.VMEM((rows * sub, 128), F32),
            pltpu.VMEM((rows * sub, 128), F32),
            pltpu.VMEM((n_state * sub, 128), F32),
            pltpu.VMEM((rows, tile), BF16),
            pltpu.VMEM((rows, dm), F32),
        ],
        compiler_params=params(),
        name="mamba",
    )(h, g, wx, cw, cb, wxp_t, dtn, bn, cn, wdt, dtb, alog_t, dsk, wz, wo)


def layer_pair(hidden, attn_norm, w_q, w_k, w_v, w_o, mlp_norm, w_gate, w_up, w_down, mamba_norm, w_in_x, w_in_z, conv_w, conv_b, w_xproj, dt_norm, b_norm, c_norm, w_dt, dt_bias, a_log, d_skip, w_out):
    dm = hidden.shape[-1]
    hd = w_q.shape[2]
    x = lax.all_to_all(hidden, "sp", 0, 1, tiled=True)
    nb, seq, _ = x.shape
    row = lambda v: v.reshape(1, -1)
    h = x.reshape(nb * seq, dm)
    h = attention(h, row(attn_norm), w_q.reshape(dm, -1), w_k.reshape(dm, -1), w_v.reshape(dm, -1), w_o.reshape(-1, dm), seq, hd)
    h = mlp(h, row(mlp_norm), w_gate, w_up, w_down)
    h = mamba(h, row(mamba_norm), w_in_x, w_in_z, conv_w, row(conv_b), w_xproj.T, row(dt_norm), row(b_norm), row(c_norm), w_dt, row(dt_bias), a_log.T, row(d_skip), w_out, seq)
    return lax.all_to_all(h.reshape(nb, seq, dm), "sp", 1, 0, tiled=True)


def solution(mesh):
    act_spec = P("dp", "sp", None)
    return jax.shard_map(
        layer_pair,
        mesh=mesh,
        in_specs=(act_spec,) + (P(),) * 23,
        out_specs=act_spec,
        check_vma=False,
    )
```

```python
import functools
import math

import jax
import jax.numpy as jnp
from jax import lax
from jax.experimental import pallas as pl
from jax.experimental.pallas import tpu as pltpu
from jax.sharding import PartitionSpec as P

EPS = 1e-6
CONV = 4
F32 = jnp.float32
BF16 = jnp.bfloat16
MESH = pl.DeviceIdType.MESH
LOG2E = 1.0 / math.log(2.0)


def dot(a, b):
    return jnp.dot(a, b, preferred_element_type=F32)


def dot_nt(a, b):
    return lax.dot_general(a, b, (((1,), (1,)), ((), ())), preferred_element_type=F32)


def rms_rows(v, gain):
    v = v.astype(F32)
    inv = lax.rsqrt(jnp.mean(v * v, axis=-1, keepdims=True) + EPS)
    return v * inv * gain.astype(F32).reshape(1, -1)


def silu(v):
    return v / (1.0 + jnp.exp(-v))


def softplus(v):
    return jnp.maximum(v, 0.0) + jnp.log1p(jnp.exp(-jnp.abs(v)))


def full(shape):
    nd = len(shape)
    return pl.BlockSpec(shape, lambda i: (0,) * nd, pipeline_mode=pl.Buffered(1))


def params(limit=60 << 20):
    return pltpu.CompilerParams(dimension_semantics=("arbitrary",), vmem_limit_bytes=limit)


def ring(n, slots, copies, body):
    for c in range(min(slots, n)):
        for cp in copies(c, c):
            cp.start()

    def run():
        def step(c, _):
            slot = lax.rem(c, slots)
            for cp in copies(c, slot):
                cp.wait()
            body(c, slot)

            @pl.when(c + slots < n)
            def _():
                for cp in copies(c + slots, slot):
                    cp.start()
            return 0
        lax.fori_loop(0, n, step, 0)
    return run


def head_kernel(n, heads, kvh, hd, x_hbm, g_ref, wq_hbm, wk_hbm, wv_hbm, wo_hbm, h_ref,
                x_s, w_s, qb_s, kvb_s, wo_s, a_s, kv_s, q_s, acc_s, pq_s, pk_s,
                ssem, rsem, lsem, qsem, kvsem, osem):
    me = lax.axis_index("sp")
    nb, seq, dm = x_s.shape
    tl = seq // n
    rows = nb * seq
    grp = heads // kvh
    tile = grp * hd
    blk = pq_s.shape[0]
    kq, kk = blk // heads, blk // kvh
    cq, ck = qb_s.shape[1] // heads, kvb_s.shape[2] // kvh

    def q_copies(c, slot):
        m = cq * heads
        return [pltpu.make_async_copy(wq_hbm.at[pl.ds(pl.multiple_of(c * m, m), m)], qb_s.at[slot], qsem.at[slot])]

    def kv_copies(c, slot):
        m = ck * kvh
        return [pltpu.make_async_copy(w.at[pl.ds(pl.multiple_of(c * m, m), m)], kvb_s.at[slot, k], kvsem.at[slot, k])
                for k, w in enumerate((wk_hbm, wv_hbm))]

    def o_copies(c, slot):
        return [pltpu.make_async_copy(wo_hbm.at[pl.ds(pl.multiple_of(c * tile, tile), tile)], wo_s.at[slot], osem.at[slot])]

    def q_body(c, slot):
        def sub(s, _):
            m = 4 * blk
            rhs = jnp.concatenate(
                [qb_s[slot, pl.ds(pl.multiple_of(s * m + i * blk, blk), blk), :] for i in range(4)], axis=1)
            y = dot(pq_s[...], rhs)
            k0 = pl.multiple_of(c * cq + s * 4 * kq, 4 * kq)
            for h in range(heads):
                for p in range(2):
                    pair = [y[h * kq:(h + 1) * kq, (2 * p + e) * hd:(2 * p + e + 1) * hd] for e in range(2)]
                    w_s[pl.ds(k0 + 2 * kq * p, 2 * kq), h * hd:(h + 1) * hd] = jnp.concatenate(pair, axis=0).astype(BF16)
            return 0
        for s in range(cq // (4 * kq)):
            sub(s, 0)

    def kv_body(c, slot):
        def sub(s, _):
            m = 2 * blk
            rhs = jnp.concatenate(
                [kvb_s[slot, k, pl.ds(pl.multiple_of(s * m + i * blk, blk), blk), :] for k in range(2) for i in range(2)], axis=1)
            y = dot(pk_s[...], rhs)
            k0 = pl.multiple_of(c * ck + s * 2 * kk, 2 * kk)
            for k in range(2):
                for i in range(2):
                    for h in range(kvh):
                        col = heads * hd + (k * kvh + h) * hd
                        w_s[pl.ds(k0 + i * kk, kk), col:col + hd] = y[h * kk:(h + 1) * kk, (2 * k + i) * hd:(2 * k + i + 1) * hd].astype(BF16)
            return 0
        for s in range(ck // (2 * kk)):
            sub(s, 0)

    run_kv = ring(dm // ck, kvb_s.shape[0], kv_copies, kv_body)
    run_q = ring(dm // cq, qb_s.shape[0], q_copies, q_body)

    bar = pltpu.get_barrier_semaphore()
    for d in range(1, n):
        pl.semaphore_signal(bar, inc=1, device_id={"sp": lax.rem(me + d, n)}, device_id_type=MESH)
    own = pltpu.make_async_copy(x_hbm.at[pl.ds(me * nb, nb)], x_s.at[:, pl.ds(pl.multiple_of(me * tl, tl), tl), :], lsem)
    own.start()
    r_i = lax.broadcasted_iota(jnp.int32, (blk, blk), 0)
    c_i = lax.broadcasted_iota(jnp.int32, (blk, blk), 1)
    pq_s[...] = jnp.where(c_i == (r_i % kq) * heads + r_i // kq, 1.0, 0.0).astype(BF16)
    pk_s[...] = jnp.where(c_i == (r_i % kk) * kvh + r_i // kk, 1.0, 0.0).astype(BF16)
    pl.semaphore_wait(bar, n - 1)
    sends = []
    half = n // 2
    for d in [half] + [v for k in range(half - 1, 0, -1) for v in (k, n - k)]:
        peer = lax.rem(me + d, n)
        cp = pltpu.make_async_remote_copy(
            src_ref=x_hbm.at[pl.ds(peer * nb, nb)], dst_ref=x_s.at[:, pl.ds(pl.multiple_of(me * tl, tl), tl), :],
            send_sem=ssem.at[d], recv_sem=rsem.at[d], device_id={"sp": peer}, device_id_type=MESH)
        cp.start()
        sends.append(cp)

    run_kv()
    run_q()
    slots_o = wo_s.shape[0]
    n_o = wo_hbm.shape[0] // tile
    for c in range(slots_o):
        for cp in o_copies(c, c):
            cp.start()
    own.wait()
    for cp in sends:
        cp.wait()

    for b in range(nb):
        xb = x_s[b]
        a_s[b * seq:(b + 1) * seq, :] = rms_rows(xb, g_ref[...]).astype(BF16)
        acc_s[b * seq:(b + 1) * seq, :] = xb.astype(F32)

    def kv_proj(c, _):
        col = pl.multiple_of(heads * hd + c * tile, tile)
        val = dot(a_s[...], w_s[:, pl.ds(col, tile)]).astype(BF16)
        for h in range(grp):
            kv_s[c * grp + h] = val[:, h * hd:(h + 1) * hd]
        return 0
    lax.fori_loop(0, 2 * kvh // grp, kv_proj, 0)

    q_s[0] = dot(a_s[...], w_s[:, 0:tile]).astype(BF16)
    row_t = lax.broadcasted_iota(jnp.int32, (grp * seq, seq), 0) % seq
    col_t = lax.broadcasted_iota(jnp.int32, (grp * seq, seq), 1)
    causal = row_t >= col_t

    def group(j, _):
        slot = lax.rem(j, slots_o)
        nxt = jnp.minimum(j + 1, n_o - 1)
        cur = lax.rem(j, 2)
        q_next = dot(a_s[...], w_s[:, pl.ds(pl.multiple_of(nxt * tile, tile), tile)]).astype(BF16)
        outs = []
        for b in range(nb):
            qb = q_s[cur, b * seq:(b + 1) * seq, :]
            q4 = jnp.concatenate([qb[:, g * hd:(g + 1) * hd] for g in range(grp)], axis=0)
            kb = kv_s[j, b * seq:(b + 1) * seq, :]
            vb = kv_s[kvh + j, b * seq:(b + 1) * seq, :]
            s = dot_nt(q4, kb) * (hd ** -0.5)
            s = jnp.where(causal, s, -jnp.inf)
            e = jnp.exp(s - jnp.max(s, axis=-1, keepdims=True))
            p = (e / jnp.sum(e, axis=-1, keepdims=True)).astype(BF16)
            o = dot(p, vb).astype(BF16)
            outs.append(jnp.concatenate([o[g * seq:(g + 1) * seq, :] for g in range(grp)], axis=1))
        q_s[1 - cur] = q_next
        for cp in o_copies(j, slot):
            cp.wait()
        acc_s[...] += dot(jnp.concatenate(outs, axis=0), wo_s[slot])

        @pl.when(j + slots_o < n_o)
        def _():
            for cp in o_copies(j + slots_o, slot):
                cp.start()
        return 0
    lax.fori_loop(0, n_o, group, 0)
    h_ref[...] = acc_s[...].astype(BF16)


def head(x, g, wq, wk, wv, wo, n):
    batch, tl, dm = x.shape
    heads, hd = wq.shape[1:]
    kvh = wk.shape[1]
    nb, seq = batch // n, tl * n
    rows = nb * seq
    grp = heads // kvh
    tile = grp * hd
    blk = 256
    cq, ck, slots_q, slots_o = 128, 320, 3, 3
    any_ = pl.BlockSpec(memory_space=pl.ANY)
    vm = pl.BlockSpec(memory_space=pltpu.VMEM)
    flat = lambda w: w.reshape(-1, w.shape[-1])
    return pl.pallas_call(
        functools.partial(head_kernel, n, heads, kvh, hd),
        out_shape=jax.ShapeDtypeStruct((rows, dm), BF16),
        in_specs=[any_, vm, any_, any_, any_, any_],
        out_specs=vm,
        scratch_shapes=[
            pltpu.VMEM((nb, seq, dm), BF16),
            pltpu.VMEM((dm, (heads + 2 * kvh) * hd), BF16),
            pltpu.VMEM((slots_q, cq * heads, hd), BF16),
            pltpu.VMEM((2, 2, ck * kvh, hd), BF16),
            pltpu.VMEM((slots_o, tile, dm), BF16),
            pltpu.VMEM((rows, dm), BF16),
            pltpu.VMEM((2 * kvh, rows, hd), BF16),
            pltpu.VMEM((2, rows, tile), BF16),
            pltpu.VMEM((rows, dm), F32),
            pltpu.VMEM((blk, blk), BF16),
            pltpu.VMEM((blk, blk), BF16),
            pltpu.SemaphoreType.DMA((n,)),
            pltpu.SemaphoreType.DMA((n,)),
            pltpu.SemaphoreType.DMA,
            pltpu.SemaphoreType.DMA((slots_q,)),
            pltpu.SemaphoreType.DMA((2, 2)),
            pltpu.SemaphoreType.DMA((slots_o,)),
        ],
        compiler_params=pltpu.CompilerParams(collective_id=0, has_side_effects=True, vmem_limit_bytes=63 << 20),
        name="head",
    )(x, g, flat(wq), flat(wk), flat(wv), flat(wo))


def mlp_kernel(h_ref, g_ref, wg_ref, wu_ref, wd_ref, o_ref, m_s, act_s, acc_s):
    i = pl.program_id(0)
    n = pl.num_programs(0) - 1

    @pl.when(i == 0)
    def _():
        m_s[...] = rms_rows(h_ref[...], g_ref[...]).astype(BF16)
        acc_s[...] = h_ref[...].astype(F32)
        gate = dot(m_s[...], wg_ref[...])
        up = dot(m_s[...], wu_ref[...])
        act_s[0] = (silu(gate) * up).astype(BF16)

    @pl.when((i > 0) & (i < n))
    def _():
        gate = dot(m_s[...], wg_ref[...])
        up = dot(m_s[...], wu_ref[...])
        acc_s[...] += dot(act_s[lax.rem(i + 1, 2)], wd_ref[...])
        act_s[lax.rem(i, 2)] = (silu(gate) * up).astype(BF16)

    @pl.when(i == n)
    def _():
        o_ref[...] = (acc_s[...] + dot(act_s[lax.rem(i + 1, 2)], wd_ref[...])).astype(BF16)


def mlp(h, g, wg, wu, wd, tile=512):
    rows, dm = h.shape
    n = wg.shape[1] // tile
    return pl.pallas_call(
        mlp_kernel,
        grid=(n + 1,),
        out_shape=jax.ShapeDtypeStruct((rows, dm), BF16),
        in_specs=[
            full((rows, dm)), full((dm,)),
            pl.BlockSpec((dm, tile), lambda i: (0, jnp.minimum(i, n - 1))),
            pl.BlockSpec((dm, tile), lambda i: (0, jnp.minimum(i, n - 1))),
            pl.BlockSpec((tile, dm), lambda i: (jnp.maximum(i - 1, 0), 0)),
        ],
        out_specs=full((rows, dm)),
        scratch_shapes=[
            pltpu.VMEM((rows, dm), BF16),
            pltpu.VMEM((2, rows, tile), BF16),
            pltpu.VMEM((rows, dm), F32),
        ],
        compiler_params=params(),
        name="mlp",
    )(h, g, wg, wu, wd)


def mamba_kernel(n, ne, seq, dt_rank, n_state, h_ref, g_ref, wx_ref, cw_ref, cb_ref, wxp_ref,
                 dtn_ref, bn_ref, cn_ref, wdt_ref, dtb_ref, alog_ref, dsk_ref, wz_ref, wo_ref, o_hbm,
                 u_s, c_s, r_s, dt_s, b_s, cc_s, d_s, x_s, y_s, a_s, st_s, z_s, gate_s, acc_s, o_s,
                 ssem, rsem, lsem):
    i = pl.program_id(0)
    last = pl.num_programs(0) - 1
    me = lax.axis_index("sp")
    rows, dm = u_s.shape
    tile = c_s.shape[2]
    sub = tile // 128
    nb = rows // seq
    tl = seq // n
    part = 256
    n_part = tile // part
    tc = seq // n_part

    @pl.when(i == 0)
    def _():
        bar = pltpu.get_barrier_semaphore()
        for d in range(1, n):
            pl.semaphore_signal(bar, inc=1, device_id={"sp": lax.rem(me + d, n)}, device_id_type=MESH)
        u_s[...] = rms_rows(h_ref[...], g_ref[...]).astype(BF16)
        acc_s[...] = h_ref[...].astype(F32)
        r_s[...] = jnp.zeros_like(r_s)
        gate_s[...] = jnp.zeros_like(gate_s)

    @pl.when(i < ne)
    def _():
        xi = dot(u_s[...], wx_ref[...]).astype(BF16).astype(F32)
        t_idx = lax.broadcasted_iota(jnp.int32, xi.shape, 0) % seq
        acc = cb_ref[...].astype(F32).reshape(1, -1) + xi * cw_ref[CONV - 1:CONV, :].astype(F32)
        for s in range(1, CONV):
            prev = jnp.where(t_idx >= s, pltpu.roll(xi, s, 0), 0.0)
            acc = acc + prev * cw_ref[CONV - 1 - s:CONV - s, :].astype(F32)
        c = silu(acc).astype(BF16)
        c_s[jnp.minimum(i, ne - 1)] = c
        r_s[...] += dot_nt(c, wxp_ref[...])

    @pl.when(i == ne - 1)
    def _():
        z_s[0] = dot(u_s[...], wz_ref[...]).astype(BF16)
        r = r_s[...]
        dt_s[...] = rms_rows(r[:, :dt_rank], dtn_ref[...]).astype(BF16)
        bm = rms_rows(r[:, dt_rank:dt_rank + n_state], bn_ref[...])
        cm = rms_rows(r[:, dt_rank + n_state:], cn_ref[...])
        for k in range(n_state):
            b_s[k] = jnp.broadcast_to(bm[:, k:k + 1], (rows, 128))
            cc_s[k] = jnp.broadcast_to(cm[:, k:k + 1], (rows, 128))

    @pl.when((i >= ne) & (i < last))
    def _():
        e = i - ne
        zc, zn = lax.rem(e, 2), lax.rem(e + 1, 2)
        delta = softplus(dot(dt_s[...], wdt_ref[...]) + dtb_ref[...])
        dx = delta * c_s[e].astype(F32)
        a2 = -jnp.exp(alog_ref[...]) * LOG2E
        for j in range(sub):
            d_s[pl.ds(j, rows, stride=sub), :] = delta[:, j * 128:(j + 1) * 128]
            x_s[pl.ds(j, rows, stride=sub), :] = dx[:, j * 128:(j + 1) * 128]
            a_s[pl.ds(j, n_state, stride=sub), :] = a2[:, j * 128:(j + 1) * 128]
        st_s[...] = jnp.zeros_like(st_s)

        def chunk(c, _):
            k0 = pl.multiple_of(c * part, part)
            z_s[zn, :, pl.ds(k0, part)] = dot(u_s[...], wz_ref[:, pl.ds(k0, part)]).astype(BF16)
            acc_s[...] += dot(gate_s[:, pl.ds(k0, part)], wo_ref[pl.ds(k0, part), :])
            for b in range(nb):
                state = [st_s[b * n_state + k] for k in range(n_state)]
                for tt in range(tc):
                    tok = b * seq + c * tc + tt
                    row = pl.multiple_of(tok * sub, sub)
                    dl = d_s[pl.ds(row, sub), :]
                    dxt = x_s[pl.ds(row, sub), :]
                    parts = [None] * 2
                    for k in range(n_state):
                        bb = b_s[k, pl.ds(tok, sub, stride=0), :]
                        ct = cc_s[k, pl.ds(tok, sub, stride=0), :]
                        s = jnp.exp2(dl * a_s[k * sub:(k + 1) * sub, :]) * state[k] + dxt * bb
                        state[k] = s
                        term = s * ct
                        parts[k % 2] = term if parts[k % 2] is None else parts[k % 2] + term
                    y_s[pl.ds(row, sub), :] = parts[0] + parts[1]
                for k in range(n_state):
                    st_s[b * n_state + k] = state[k]
            return 0

        lax.fori_loop(0, n_part, chunk, 0)
        for j in range(sub):
            lanes = slice(j * 128, (j + 1) * 128)
            y = y_s[pl.ds(j, rows, stride=sub), :] + dsk_ref[:, lanes] * c_s[e, :, lanes].astype(F32)
            gate_s[:, lanes] = (y * silu(z_s[zc, :, lanes].astype(F32))).astype(BF16)

    @pl.when(i == last)
    def _():
        n_out = o_s.shape[0]
        w = o_s.shape[3]
        pl.semaphore_wait(pltpu.get_barrier_semaphore(), n - 1)
        half = n // 2
        order = [half] + [v for k in range(half - 1, 0, -1) for v in (k, n - k)]
        copies = []

        def send(q):
            lanes = slice(q * w, (q + 1) * w)
            for d in order:
                peer = lax.rem(me + d, n)
                cp = pltpu.make_async_remote_copy(
                    src_ref=o_s.at[q, :, pl.ds(pl.multiple_of(peer * tl, tl), tl), :],
                    dst_ref=o_hbm.at[pl.ds(me * nb, nb), :, lanes],
                    send_sem=ssem.at[q, d], recv_sem=rsem.at[q, d], device_id={"sp": peer}, device_id_type=MESH)
                cp.start()
                copies.append(cp)
            cp = pltpu.make_async_copy(o_s.at[q, :, pl.ds(pl.multiple_of(me * tl, tl), tl), :],
                                       o_hbm.at[pl.ds(me * nb, nb), :, lanes], lsem.at[q])
            cp.start()
            copies.append(cp)

        for q in range(n_out):
            lanes = slice(q * w, (q + 1) * w)
            val = (acc_s[:, lanes] + dot(gate_s[...], wo_ref[:, lanes])).astype(BF16)
            for b in range(nb):
                o_s[q, b] = val[b * seq:(b + 1) * seq, :]
            if q:
                send(q - 1)
        send(n_out - 1)
        for cp in copies:
            cp.wait()


def mamba(h, g, wx, wz, cw, cb, wxp_t, dtn, bn, cn, wdt, dtb, alog_t, dsk, wo, seq, n, tile=1024, n_out=5):
    rows, dm = h.shape
    inner = wx.shape[1]
    dt_rank, n_state = wdt.shape[0], alog_t.shape[0]
    nr = wxp_t.shape[0]
    ne = inner // tile
    sub = tile // 128
    nb, tl = rows // seq, seq // n
    pa = lambda i: (0, jnp.minimum(i, ne - 1))
    pb = lambda i: (0, jnp.clip(i - ne, 0, ne - 1))
    return pl.pallas_call(
        functools.partial(mamba_kernel, n, ne, seq, dt_rank, n_state),
        grid=(2 * ne + 1,),
        out_shape=jax.ShapeDtypeStruct((nb * n, tl, dm), BF16),
        in_specs=[
            full((rows, dm)), full((dm,)),
            pl.BlockSpec((dm, tile), pa),
            pl.BlockSpec((CONV, tile), pa),
            pl.BlockSpec((tile,), lambda i: (jnp.minimum(i, ne - 1),)),
            pl.BlockSpec((nr, tile), pa),
            full((1, dt_rank)), full((1, n_state)), full((1, n_state)),
            pl.BlockSpec((dt_rank, tile), pb),
            pl.BlockSpec((1, tile), pb),
            pl.BlockSpec((n_state, tile), pb),
            pl.BlockSpec((1, tile), pb),
            pl.BlockSpec((dm, tile), lambda i: (0, jnp.clip(i - ne + 1, 0, ne - 1))),
            pl.BlockSpec((tile, dm), lambda i: (jnp.clip(i - ne - 1, 0, ne - 1), 0)),
        ],
        out_specs=pl.BlockSpec(memory_space=pl.ANY),
        scratch_shapes=[
            pltpu.VMEM((rows, dm), BF16),
            pltpu.VMEM((ne, rows, tile), BF16),
            pltpu.VMEM((rows, nr), F32),
            pltpu.VMEM((rows, dt_rank), BF16),
            pltpu.VMEM((n_state, rows, 128), F32),
            pltpu.VMEM((n_state, rows, 128), F32),
            pltpu.VMEM((rows * sub, 128), F32),
            pltpu.VMEM((rows * sub, 128), F32),
            pltpu.VMEM((rows * sub, 128), F32),
            pltpu.VMEM((n_state * sub, 128), F32),
            pltpu.VMEM((nb * n_state, sub, 128), F32),
            pltpu.VMEM((2, rows, tile), BF16),
            pltpu.VMEM((rows, tile), BF16),
            pltpu.VMEM((rows, dm), F32),
            pltpu.VMEM((n_out, nb, seq, dm // n_out), BF16),
            pltpu.SemaphoreType.DMA((n_out, n)),
            pltpu.SemaphoreType.DMA((n_out, n)),
            pltpu.SemaphoreType.DMA((n_out,)),
        ],
        compiler_params=pltpu.CompilerParams(dimension_semantics=("arbitrary",), collective_id=1, has_side_effects=True, vmem_limit_bytes=63 << 20),
        name="mamba",
    )(h, g, wx, cw, cb, wxp_t, dtn, bn, cn, wdt, dtb, alog_t, dsk, wz, wo)


def layer_pair(hidden, attn_norm, w_q, w_k, w_v, w_o, mlp_norm, w_gate, w_up, w_down, mamba_norm, w_in_x, w_in_z, conv_w, conv_b, w_xproj, dt_norm, b_norm, c_norm, w_dt, dt_bias, a_log, d_skip, w_out, n_shards):
    batch, tl, dm = hidden.shape
    seq = tl * n_shards
    row = lambda v: v.reshape(1, -1)
    h = head(hidden, attn_norm, w_q, w_k, w_v, w_o, n_shards)
    h = mlp(h, mlp_norm, w_gate, w_up, w_down)
    return mamba(h, mamba_norm, w_in_x, w_in_z, conv_w, conv_b, w_xproj.T, row(dt_norm), row(b_norm), row(c_norm), w_dt, row(dt_bias), a_log.T, row(d_skip), w_out, seq, n_shards)


def solution(mesh):
    act_spec = P("dp", "sp", None)
    return jax.shard_map(
        functools.partial(layer_pair, n_shards=mesh.shape["sp"]),
        mesh=mesh,
        in_specs=(act_spec,) + (P(),) * 23,
        out_specs=act_spec,
        check_vma=False,
    )
```

```python
import functools
import math

import jax
import jax.numpy as jnp
from jax import lax
from jax.experimental import pallas as pl
from jax.experimental.pallas import tpu as pltpu
from jax.sharding import PartitionSpec as P

EPS = 1e-6
CONV = 4
F32 = jnp.float32
BF16 = jnp.bfloat16
MESH = pl.DeviceIdType.MESH
LOG2E = 1.0 / math.log(2.0)


def dot(a, b):
    return jnp.dot(a, b, preferred_element_type=F32)


def dot_nt(a, b):
    return lax.dot_general(a, b, (((1,), (1,)), ((), ())), preferred_element_type=F32)


def rms_rows(v, gain):
    v = v.astype(F32)
    inv = lax.rsqrt(jnp.mean(v * v, axis=-1, keepdims=True) + EPS)
    return v * inv * gain.astype(F32).reshape(1, -1)


def silu(v):
    return v / (1.0 + jnp.exp(-v))


def softplus(v):
    return jnp.maximum(v, 0.0) + jnp.log1p(jnp.exp(-jnp.abs(v)))


def ring(n, slots, copies, body):
    for c in range(min(slots, n)):
        for cp in copies(c, c):
            cp.start()

    def run():
        def step(c, _):
            slot = lax.rem(c, slots)
            for cp in copies(c, slot):
                cp.wait()
            body(c, slot)

            @pl.when(c + slots < n)
            def _():
                for cp in copies(c + slots, slot):
                    cp.start()
            return 0
        lax.fori_loop(0, n, step, 0)
    return run


def head_kernel(n, heads, kvh, hd, x_hbm, g_ref, wq_hbm, wk_hbm, wv_hbm, wo_hbm, h_ref,
                x_s, w_s, qb_s, kvb_s, wo_s, a_s, kv_s, q_s, acc_s, pq_s, pk_s,
                ssem, rsem, lsem, qsem, kvsem, osem):
    me = lax.axis_index("sp")
    nb, seq, dm = x_s.shape
    tl = seq // n
    rows = nb * seq
    grp = heads // kvh
    tile = grp * hd
    blk = pq_s.shape[0]
    kq, kk = blk // heads, blk // kvh
    cq, ck = qb_s.shape[1] // heads, kvb_s.shape[2] // kvh

    def q_copies(c, slot):
        m = cq * heads
        return [pltpu.make_async_copy(wq_hbm.at[pl.ds(pl.multiple_of(c * m, m), m)], qb_s.at[slot], qsem.at[slot])]

    def kv_copies(c, slot):
        m = ck * kvh
        return [pltpu.make_async_copy(w.at[pl.ds(pl.multiple_of(c * m, m), m)], kvb_s.at[slot, k], kvsem.at[slot, k])
                for k, w in enumerate((wk_hbm, wv_hbm))]

    def o_copies(c, slot):
        return [pltpu.make_async_copy(wo_hbm.at[pl.ds(pl.multiple_of(c * tile, tile), tile)], wo_s.at[slot], osem.at[slot])]

    def q_body(c, slot):
        def sub(s, _):
            m = 4 * blk
            rhs = jnp.concatenate(
                [qb_s[slot, pl.ds(pl.multiple_of(s * m + i * blk, blk), blk), :] for i in range(4)], axis=1)
            y = dot(pq_s[...], rhs)
            k0 = pl.multiple_of(c * cq + s * 4 * kq, 4 * kq)
            for h in range(heads):
                for p in range(2):
                    pair = [y[h * kq:(h + 1) * kq, (2 * p + e) * hd:(2 * p + e + 1) * hd] for e in range(2)]
                    w_s[pl.ds(k0 + 2 * kq * p, 2 * kq), h * hd:(h + 1) * hd] = jnp.concatenate(pair, axis=0).astype(BF16)
            return 0
        for s in range(cq // (4 * kq)):
            sub(s, 0)

    def kv_body(c, slot):
        def sub(s, _):
            m = 2 * blk
            rhs = jnp.concatenate(
                [kvb_s[slot, k, pl.ds(pl.multiple_of(s * m + i * blk, blk), blk), :] for k in range(2) for i in range(2)], axis=1)
            y = dot(pk_s[...], rhs)
            k0 = pl.multiple_of(c * ck + s * 2 * kk, 2 * kk)
            for k in range(2):
                for i in range(2):
                    for h in range(kvh):
                        col = heads * hd + (k * kvh + h) * hd
                        w_s[pl.ds(k0 + i * kk, kk), col:col + hd] = y[h * kk:(h + 1) * kk, (2 * k + i) * hd:(2 * k + i + 1) * hd].astype(BF16)
            return 0
        for s in range(ck // (2 * kk)):
            sub(s, 0)

    run_kv = ring(dm // ck, kvb_s.shape[0], kv_copies, kv_body)
    run_q = ring(dm // cq, qb_s.shape[0], q_copies, q_body)

    bar = pltpu.get_barrier_semaphore()
    for d in range(1, n):
        pl.semaphore_signal(bar, inc=1, device_id={"sp": lax.rem(me + d, n)}, device_id_type=MESH)
    own = pltpu.make_async_copy(x_hbm.at[pl.ds(me * nb, nb)], x_s.at[:, pl.ds(pl.multiple_of(me * tl, tl), tl), :], lsem)
    own.start()
    r_i = lax.broadcasted_iota(jnp.int32, (blk, blk), 0)
    c_i = lax.broadcasted_iota(jnp.int32, (blk, blk), 1)
    pq_s[...] = jnp.where(c_i == (r_i % kq) * heads + r_i // kq, 1.0, 0.0).astype(BF16)
    pk_s[...] = jnp.where(c_i == (r_i % kk) * kvh + r_i // kk, 1.0, 0.0).astype(BF16)
    pl.semaphore_wait(bar, n - 1)
    sends = []
    half = n // 2
    for d in [half] + [v for k in range(half - 1, 0, -1) for v in (k, n - k)]:
        peer = lax.rem(me + d, n)
        cp = pltpu.make_async_remote_copy(
            src_ref=x_hbm.at[pl.ds(peer * nb, nb)], dst_ref=x_s.at[:, pl.ds(pl.multiple_of(me * tl, tl), tl), :],
            send_sem=ssem.at[d], recv_sem=rsem.at[d], device_id={"sp": peer}, device_id_type=MESH)
        cp.start()
        sends.append(cp)

    run_kv()
    run_q()
    slots_o = wo_s.shape[0]
    n_o = wo_hbm.shape[0] // tile
    for c in range(slots_o):
        for cp in o_copies(c, c):
            cp.start()
    own.wait()
    for cp in sends:
        cp.wait()

    for b in range(nb):
        xb = x_s[b]
        a_s[b * seq:(b + 1) * seq, :] = rms_rows(xb, g_ref[...]).astype(BF16)
        acc_s[b * seq:(b + 1) * seq, :] = xb.astype(F32)

    def kv_proj(c, _):
        col = pl.multiple_of(heads * hd + c * tile, tile)
        val = dot(a_s[...], w_s[:, pl.ds(col, tile)]).astype(BF16)
        for h in range(grp):
            kv_s[c * grp + h] = val[:, h * hd:(h + 1) * hd]
        return 0
    lax.fori_loop(0, 2 * kvh // grp, kv_proj, 0)

    q_s[0] = dot(a_s[...], w_s[:, 0:tile]).astype(BF16)
    row_t = lax.broadcasted_iota(jnp.int32, (grp * seq, seq), 0) % seq
    col_t = lax.broadcasted_iota(jnp.int32, (grp * seq, seq), 1)
    causal = row_t >= col_t

    def group(j, _):
        slot = lax.rem(j, slots_o)
        nxt = jnp.minimum(j + 1, n_o - 1)
        cur = lax.rem(j, 2)
        q_next = dot(a_s[...], w_s[:, pl.ds(pl.multiple_of(nxt * tile, tile), tile)]).astype(BF16)
        outs = []
        for b in range(nb):
            qb = q_s[cur, b * seq:(b + 1) * seq, :]
            q4 = jnp.concatenate([qb[:, g * hd:(g + 1) * hd] for g in range(grp)], axis=0)
            kb = kv_s[j, b * seq:(b + 1) * seq, :]
            vb = kv_s[kvh + j, b * seq:(b + 1) * seq, :]
            s = dot_nt(q4, kb) * (hd ** -0.5)
            s = jnp.where(causal, s, -jnp.inf)
            e = jnp.exp(s - jnp.max(s, axis=-1, keepdims=True))
            p = (e / jnp.sum(e, axis=-1, keepdims=True)).astype(BF16)
            o = dot(p, vb).astype(BF16)
            outs.append(jnp.concatenate([o[g * seq:(g + 1) * seq, :] for g in range(grp)], axis=1))
        q_s[1 - cur] = q_next
        for cp in o_copies(j, slot):
            cp.wait()
        acc_s[...] += dot(jnp.concatenate(outs, axis=0), wo_s[slot])

        @pl.when(j + slots_o < n_o)
        def _():
            for cp in o_copies(j + slots_o, slot):
                cp.start()
        return 0
    lax.fori_loop(0, n_o, group, 0)
    h_ref[...] = acc_s[...].astype(BF16)


def head(x, g, wq, wk, wv, wo, n):
    batch, tl, dm = x.shape
    heads, hd = wq.shape[1:]
    kvh = wk.shape[1]
    nb, seq = batch // n, tl * n
    rows = nb * seq
    grp = heads // kvh
    tile = grp * hd
    blk = 256
    cq, ck, slots_q, slots_o = 128, 320, 3, 3
    any_ = pl.BlockSpec(memory_space=pl.ANY)
    vm = pl.BlockSpec(memory_space=pltpu.VMEM)
    flat = lambda w: w.reshape(-1, w.shape[-1])
    return pl.pallas_call(
        functools.partial(head_kernel, n, heads, kvh, hd),
        out_shape=jax.ShapeDtypeStruct((rows, dm), BF16),
        in_specs=[any_, vm, any_, any_, any_, any_],
        out_specs=vm,
        scratch_shapes=[
            pltpu.VMEM((nb, seq, dm), BF16),
            pltpu.VMEM((dm, (heads + 2 * kvh) * hd), BF16),
            pltpu.VMEM((slots_q, cq * heads, hd), BF16),
            pltpu.VMEM((2, 2, ck * kvh, hd), BF16),
            pltpu.VMEM((slots_o, tile, dm), BF16),
            pltpu.VMEM((rows, dm), BF16),
            pltpu.VMEM((2 * kvh, rows, hd), BF16),
            pltpu.VMEM((2, rows, tile), BF16),
            pltpu.VMEM((rows, dm), F32),
            pltpu.VMEM((blk, blk), BF16),
            pltpu.VMEM((blk, blk), BF16),
            pltpu.SemaphoreType.DMA((n,)),
            pltpu.SemaphoreType.DMA((n,)),
            pltpu.SemaphoreType.DMA,
            pltpu.SemaphoreType.DMA((slots_q,)),
            pltpu.SemaphoreType.DMA((2, 2)),
            pltpu.SemaphoreType.DMA((slots_o,)),
        ],
        compiler_params=pltpu.CompilerParams(collective_id=0, has_side_effects=True, vmem_limit_bytes=63 << 20),
        name="head",
    )(x, g, flat(wq), flat(wk), flat(wv), flat(wo))


def zero_of(vals):
    return jnp.maximum(functools.reduce(jnp.minimum, vals, jnp.zeros_like(vals[0])), 0.0)


def tail_kernel(n, seq, dt_rank, n_state, h_ref, mg_ref, wg_hbm, wu_hbm, wd_hbm, ug_ref, wx_hbm, cw_ref, cb_ref, wxp_hbm,
                dtn_ref, bn_ref, cn_ref, wdt_hbm, dtb_ref, alog_ref, dsk_ref, wz_hbm, wo_hbm, o_hbm,
                w_s, d_s, u_s, acc_s, act_s, c_s, xi_s, r_s, dt_s, b_s, cc_s, dl_s, dx_s, y_s, a_s, st_s, z_s, gate_s, o_s,
                wxp_s, wdt_s, wsem, dsem, psem, ssem, rsem, lsem):
    me = lax.axis_index("sp")
    rows, dm = u_s.shape
    slots, _, _, half_w = w_s.shape
    slots_d = d_s.shape[0]
    tile = 2 * half_w
    ne, nf = wx_hbm.shape[1] // tile, wg_hbm.shape[1] // half_w
    sub = tile // 128
    nb, tl = rows // seq, seq // n
    part = 256
    n_part = tile // part
    per = half_w // part
    tc = seq // n_part

    bar = pltpu.get_barrier_semaphore()
    for d in range(1, n):
        pl.semaphore_signal(bar, inc=1, device_id={"sp": lax.rem(me + d, n)}, device_id_type=MESH)

    def w_pair(k, a, b, ka, kb):
        slot = lax.rem(k, slots)
        return [pltpu.make_async_copy(w.at[:, pl.ds(pl.multiple_of(q * half_w, half_w), half_w)], w_s.at[slot, r], wsem.at[slot, r])
                for r, (w, q) in enumerate(((a, ka), (b, kb)))]

    def w_start(k):
        @pl.when(k < nf)
        def _():
            for cp in w_pair(k, wg_hbm, wu_hbm, k, k):
                cp.start()

        @pl.when((k >= nf) & (k < nf + ne))
        def _():
            for cp in w_pair(k, wx_hbm, wx_hbm, 2 * (k - nf), 2 * (k - nf) + 1):
                cp.start()

        @pl.when((k >= nf + ne) & (k < nf + 2 * ne))
        def _():
            for cp in w_pair(k, wz_hbm, wz_hbm, 2 * (k - nf - ne), 2 * (k - nf - ne) + 1):
                cp.start()

    def w_wait(k):
        for cp in w_pair(k, wg_hbm, wu_hbm, 0, 0):
            cp.wait()

    def d_copy(k, w, q):
        slot = lax.rem(k, slots_d)
        return pltpu.make_async_copy(w.at[pl.ds(pl.multiple_of(q * half_w, half_w), half_w)], d_s.at[slot], dsem.at[slot])

    def d_start(k):
        @pl.when(k < nf)
        def _():
            d_copy(k, wd_hbm, k).start()

        @pl.when((k >= nf) & (k < nf + 2 * ne))
        def _():
            d_copy(k, wo_hbm, k - nf).start()

    def d_wait(k):
        d_copy(k, wd_hbm, 0).wait()

    for k in range(max(slots, slots_d)):
        if k < slots:
            w_start(k)
        if k < slots_d:
            d_start(k)
    small = [pltpu.make_async_copy(wxp_hbm, wxp_s, psem.at[0]), pltpu.make_async_copy(wdt_hbm, wdt_s, psem.at[1])]
    for cp in small:
        cp.start()

    u_s[...] = rms_rows(h_ref[...], mg_ref[...]).astype(BF16)
    acc_s[...] = h_ref[...].astype(F32)
    w_wait(0)
    act_s[0] = (silu(dot(u_s[...], w_s[0, 0])) * dot(u_s[...], w_s[0, 1])).astype(BF16)
    w_start(slots)

    def ff(k, _):
        slot, prev = lax.rem(k, slots), lax.rem(k - 1, slots_d)
        w_wait(k)
        d_wait(k - 1)
        gate = dot(u_s[...], w_s[slot, 0])
        up = dot(u_s[...], w_s[slot, 1])
        acc_s[...] += dot(act_s[lax.rem(k + 1, 2)], d_s[prev])
        act_s[lax.rem(k, 2)] = (silu(gate) * up).astype(BF16)
        w_start(k + slots)
        d_start(k - 1 + slots_d)
        return 0
    lax.fori_loop(1, nf, ff, 0)
    d_wait(nf - 1)
    h2 = (acc_s[...] + dot(act_s[(nf - 1) % 2], d_s[(nf - 1) % slots_d])).astype(BF16)
    d_start(nf - 1 + slots_d)
    acc_s[...] = h2.astype(F32)
    u_s[...] = rms_rows(acc_s[...], ug_ref[...]).astype(BF16)

    r_s[...] = jnp.zeros_like(r_s)
    gate_s[...] = jnp.zeros_like(gate_s)

    def in_proj(e):
        k = nf + e
        slot = lax.rem(k, slots)
        w_wait(k)
        for r in range(2):
            xi_s[lax.rem(e, 2), :, r * half_w:(r + 1) * half_w] = dot(u_s[...], w_s[slot, r]).astype(BF16)

    def conv(e):
        col = pl.ds(pl.multiple_of(e * tile, tile), tile)
        xi = xi_s[lax.rem(e, 2)].astype(F32)
        t_idx = lax.broadcasted_iota(jnp.int32, xi.shape, 0) % seq
        acc = cb_ref[col].astype(F32).reshape(1, -1) + xi * cw_ref[CONV - 1:CONV, col].astype(F32)
        for s in range(1, CONV):
            prev = jnp.where(t_idx >= s, pltpu.roll(xi, s, 0), 0.0)
            acc = acc + prev * cw_ref[CONV - 1 - s:CONV - s, col].astype(F32)
        c = silu(acc).astype(BF16)
        c_s[e] = c
        r_s[...] += dot_nt(c, wxp_s[:, col])

    in_proj(0)
    w_start(nf + slots)
    for cp in small:
        cp.wait()

    def phase_a(e, _):
        in_proj(e)
        conv(e - 1)
        w_start(nf + e + slots)
        return 0
    lax.fori_loop(1, ne, phase_a, 0)

    kz = nf + ne
    w_wait(kz)
    for r in range(2):
        z_s[0, :, r * half_w:(r + 1) * half_w] = dot(u_s[...], w_s[kz % slots, r]).astype(BF16)
    conv(ne - 1)
    w_start(kz + slots)

    r = r_s[...]
    dt_s[...] = rms_rows(r[:, :dt_rank], dtn_ref[...]).astype(BF16)
    bm = rms_rows(r[:, dt_rank:dt_rank + n_state], bn_ref[...])
    cm = rms_rows(r[:, dt_rank + n_state:], cn_ref[...])
    for k in range(n_state):
        b_s[k] = jnp.broadcast_to(bm[:, k:k + 1], (rows, 128))
        cc_s[k] = jnp.broadcast_to(cm[:, k:k + 1], (rows, 128))

    def phase_b(e, _):
        col = pl.ds(pl.multiple_of(e * tile, tile), tile)
        zc, zn = lax.rem(e, 2), lax.rem(e + 1, 2)
        z_tile, o_tile = jnp.minimum(e + 1, ne - 1), jnp.maximum(e - 1, 0)
        slot_z = lax.rem(kz + z_tile, slots)

        @pl.when(e + 1 < ne)
        def _():
            w_wait(kz + e + 1)

        @pl.when(e != 1)
        def _():
            for q in range(2):
                d_wait(nf + 2 * o_tile + q)

        delta = softplus(dot(dt_s[...], wdt_s[:, col]) + dtb_ref[:, col])
        dx = delta * c_s[e].astype(F32)
        a2 = -jnp.exp(alog_ref[:, col]) * LOG2E
        for j in range(sub):
            dl_s[pl.ds(j, rows, stride=sub), :] = delta[:, j * 128:(j + 1) * 128]
            dx_s[pl.ds(j, rows, stride=sub), :] = dx[:, j * 128:(j + 1) * 128]
            a_s[pl.ds(j, n_state, stride=sub), :] = a2[:, j * 128:(j + 1) * 128]
        st_s[...] = jnp.zeros_like(st_s)

        def chunk(c, _):
            k0 = pl.multiple_of(c * part, part)
            kp = pl.multiple_of(lax.rem(c, per) * part, part)
            zv = dot(u_s[...], w_s[slot_z, c // per, :, pl.ds(kp, part)])
            z_s[zn, :, pl.ds(k0, part)] = zv.astype(BF16)
            slot_o = lax.rem(nf + 2 * o_tile + c // per, slots_d)
            ov = dot(gate_s[:, pl.ds(k0, part)], d_s[slot_o, pl.ds(kp, part), :])
            acc_s[...] += ov
            after_z = zero_of([zv[r0:r0 + 8, l0:l0 + 128] for r0 in (0, rows - 8) for l0 in (0, part - 128)])
            after_o = zero_of([ov[rows - 8:, l0:l0 + 128] for l0 in range(0, dm, 256)])
            for b in range(nb):
                state = [st_s[b * n_state + k] for k in range(n_state)]
                for tt in range(tc):
                    tok = b * seq + c * tc + tt
                    row = pl.multiple_of(tok * sub, sub)
                    dl = dl_s[pl.ds(row, sub), :]
                    dxt = dx_s[pl.ds(row, sub), :]
                    if b == nb - 1 and tt == 0:
                        dl = dl + after_z
                    if b == nb - 1 and tt == tc - 8:
                        dl = dl + after_o
                    parts = [None] * 2
                    for k in range(n_state):
                        bb = b_s[k, pl.ds(tok, sub, stride=0), :]
                        ct = cc_s[k, pl.ds(tok, sub, stride=0), :]
                        s = jnp.exp2(dl * a_s[k * sub:(k + 1) * sub, :]) * state[k] + dxt * bb
                        state[k] = s
                        term = s * ct
                        parts[k % 2] = term if parts[k % 2] is None else parts[k % 2] + term
                    y_s[pl.ds(row, sub), :] = parts[0] + parts[1]
                for k in range(n_state):
                    st_s[b * n_state + k] = state[k]
            return 0

        lax.fori_loop(0, n_part, chunk, 0)
        w_start(kz + e + 1 + slots)

        @pl.when(e >= 1)
        def _():
            for q in range(2):
                d_start(nf + 2 * (e - 1) + q + slots_d)

        for j in range(sub):
            lanes = slice(j * 128, (j + 1) * 128)
            dlanes = pl.ds(pl.multiple_of(e * tile + j * 128, 128), 128)
            y = y_s[pl.ds(j, rows, stride=sub), :] + dsk_ref[:, dlanes] * c_s[e, :, lanes].astype(F32)
            gate_s[:, lanes] = (y * silu(z_s[zc, :, lanes].astype(F32))).astype(BF16)
        return 0
    lax.fori_loop(0, ne, phase_b, 0)

    n_out, _, _, w = o_s.shape
    pl.semaphore_wait(bar, n - 1)
    half = n // 2
    order = [half] + [v for k in range(half - 1, 0, -1) for v in (k, n - k)]
    copies = []

    def send(q):
        lanes = slice(q * w, (q + 1) * w)
        for d in order:
            peer = lax.rem(me + d, n)
            cp = pltpu.make_async_remote_copy(
                src_ref=o_s.at[q, :, pl.ds(pl.multiple_of(peer * tl, tl), tl), :],
                dst_ref=o_hbm.at[pl.ds(me * nb, nb), :, lanes],
                send_sem=ssem.at[q, d], recv_sem=rsem.at[q, d], device_id={"sp": peer}, device_id_type=MESH)
            cp.start()
            copies.append(cp)
        cp = pltpu.make_async_copy(o_s.at[q, :, pl.ds(pl.multiple_of(me * tl, tl), tl), :],
                                   o_hbm.at[pl.ds(me * nb, nb), :, lanes], lsem.at[q])
        cp.start()
        copies.append(cp)

    for q in range(2):
        d_wait(nf + 2 * (ne - 1) + q)
    s0, s1 = [(nf + 2 * (ne - 1) + q) % slots_d for q in range(2)]
    for q in range(n_out):
        lanes = slice(q * w, (q + 1) * w)
        val = acc_s[:, lanes] + dot(gate_s[:, :half_w], d_s[s0, :, lanes]) + dot(gate_s[:, half_w:], d_s[s1, :, lanes])
        for b in range(nb):
            o_s[q, b] = val[b * seq:(b + 1) * seq, :].astype(BF16)
        if q:
            send(q - 1)
    send(n_out - 1)
    for cp in copies:
        cp.wait()


def tail(h, mg, wg, wu, wd, ug, wx, wz, cw, cb, wxp_t, dtn, bn, cn, wdt, dtb, alog_t, dsk, wo, seq, n, half_w=512, n_out=5, slots=3, slots_d=4):
    rows, dm = h.shape
    inner = wx.shape[1]
    dt_rank, n_state = wdt.shape[0], alog_t.shape[0]
    nr = wxp_t.shape[0]
    tile = 2 * half_w
    ne = inner // tile
    sub = tile // 128
    nb, tl = rows // seq, seq // n
    any_ = pl.BlockSpec(memory_space=pl.ANY)
    vm = pl.BlockSpec(memory_space=pltpu.VMEM)
    return pl.pallas_call(
        functools.partial(tail_kernel, n, seq, dt_rank, n_state),
        out_shape=jax.ShapeDtypeStruct((nb * n, tl, dm), BF16),
        in_specs=[vm, vm, any_, any_, any_, vm, any_, vm, vm, any_, vm, vm, vm, any_, vm, vm, vm, any_, any_],
        out_specs=any_,
        scratch_shapes=[
            pltpu.VMEM((slots, 2, dm, half_w), BF16),
            pltpu.VMEM((slots_d, half_w, dm), BF16),
            pltpu.VMEM((rows, dm), BF16),
            pltpu.VMEM((rows, dm), F32),
            pltpu.VMEM((2, rows, half_w), BF16),
            pltpu.VMEM((ne, rows, tile), BF16),
            pltpu.VMEM((2, rows, tile), BF16),
            pltpu.VMEM((rows, nr), F32),
            pltpu.VMEM((rows, dt_rank), BF16),
            pltpu.VMEM((n_state, rows, 128), F32),
            pltpu.VMEM((n_state, rows, 128), F32),
            pltpu.VMEM((rows * sub, 128), F32),
            pltpu.VMEM((rows * sub, 128), F32),
            pltpu.VMEM((rows * sub, 128), F32),
            pltpu.VMEM((n_state * sub, 128), F32),
            pltpu.VMEM((nb * n_state, sub, 128), F32),
            pltpu.VMEM((2, rows, tile), BF16),
            pltpu.VMEM((rows, tile), BF16),
            pltpu.VMEM((n_out, nb, seq, dm // n_out), BF16),
            pltpu.VMEM((nr, inner), BF16),
            pltpu.VMEM((dt_rank, inner), BF16),
            pltpu.SemaphoreType.DMA((slots, 2)),
            pltpu.SemaphoreType.DMA((slots_d,)),
            pltpu.SemaphoreType.DMA((2,)),
            pltpu.SemaphoreType.DMA((n_out, n)),
            pltpu.SemaphoreType.DMA((n_out, n)),
            pltpu.SemaphoreType.DMA((n_out,)),
        ],
        compiler_params=pltpu.CompilerParams(collective_id=1, has_side_effects=True, vmem_limit_bytes=63 << 20),
        name="tail",
    )(h, mg, wg, wu, wd, ug, wx, cw, cb, wxp_t, dtn, bn, cn, wdt, dtb, alog_t, dsk, wz, wo)


def layer_pair(hidden, attn_norm, w_q, w_k, w_v, w_o, mlp_norm, w_gate, w_up, w_down, mamba_norm, w_in_x, w_in_z, conv_w, conv_b, w_xproj, dt_norm, b_norm, c_norm, w_dt, dt_bias, a_log, d_skip, w_out, n_shards):
    batch, tl, dm = hidden.shape
    seq = tl * n_shards
    row = lambda v: v.reshape(1, -1)
    h = head(hidden, attn_norm, w_q, w_k, w_v, w_o, n_shards)
    return tail(h, mlp_norm, w_gate, w_up, w_down, mamba_norm, w_in_x, w_in_z, conv_w, conv_b, w_xproj.T, row(dt_norm), row(b_norm), row(c_norm), w_dt, row(dt_bias), a_log.T, row(d_skip), w_out, seq, n_shards)


def solution(mesh):
    act_spec = P("dp", "sp", None)
    return jax.shard_map(
        functools.partial(layer_pair, n_shards=mesh.shape["sp"]),
        mesh=mesh,
        in_specs=(act_spec,) + (P(),) * 23,
        out_specs=act_spec,
        check_vma=False,
    )
```

```python
import functools
import math

import jax
import jax.numpy as jnp
from jax import lax
from jax.experimental import pallas as pl
from jax.experimental.pallas import tpu as pltpu
from jax.sharding import PartitionSpec as P

EPS = 1e-6
CONV = 4
LAG = 20
F32 = jnp.float32
BF16 = jnp.bfloat16
MESH = pl.DeviceIdType.MESH
LOG2E = 1.0 / math.log(2.0)


def dot(a, b):
    return jnp.dot(a, b, preferred_element_type=F32)


def dot_nt(a, b):
    return lax.dot_general(a, b, (((1,), (1,)), ((), ())), preferred_element_type=F32)


def rms_rows(v, gain):
    v = v.astype(F32)
    inv = lax.rsqrt(jnp.mean(v * v, axis=-1, keepdims=True) + EPS)
    return v * inv * gain.astype(F32).reshape(1, -1)


def silu(v):
    return v / (1.0 + jnp.exp(-v))


def softplus(v):
    w = jnp.exp(-jnp.abs(v))
    u = 1.0 + w
    return jnp.maximum(v, 0.0) + (jnp.log(u) + (w - (u - 1.0)))


def ring(n, slots, copies, body):
    for c in range(min(slots, n)):
        for cp in copies(c, c):
            cp.start()

    def run():
        def step(c, _):
            slot = lax.rem(c, slots)
            for cp in copies(c, slot):
                cp.wait()
            body(c, slot)

            @pl.when(c + slots < n)
            def _():
                for cp in copies(c + slots, slot):
                    cp.start()
            return 0
        lax.fori_loop(0, n, step, 0)
    return run


def head_kernel(n, heads, kvh, hd, x_hbm, g_ref, wq_hbm, wk_hbm, wv_hbm, wo_hbm, h_ref,
                x_s, w_s, qb_s, kvb_s, wo_s, a_s, kv_s, q_s, acc_s, pq_s, pk_s,
                ssem, rsem, lsem, qsem, kvsem, osem):
    me = lax.axis_index("sp")
    nb, seq, dm = x_s.shape
    tl = seq // n
    rows = nb * seq
    grp = heads // kvh
    tile = grp * hd
    blk = pq_s.shape[0]
    kq, kk = blk // heads, blk // kvh
    cq, ck = qb_s.shape[1] // heads, kvb_s.shape[2] // kvh

    def q_copies(c, slot):
        m = cq * heads
        return [pltpu.make_async_copy(wq_hbm.at[pl.ds(pl.multiple_of(c * m, m), m)], qb_s.at[slot], qsem.at[slot])]

    def kv_copies(c, slot):
        m = ck * kvh
        return [pltpu.make_async_copy(w.at[pl.ds(pl.multiple_of(c * m, m), m)], kvb_s.at[slot, k], kvsem.at[slot, k])
                for k, w in enumerate((wk_hbm, wv_hbm))]

    def o_copies(c, slot):
        return [pltpu.make_async_copy(wo_hbm.at[pl.ds(pl.multiple_of(c * tile, tile), tile)], wo_s.at[slot], osem.at[slot])]

    def q_body(c, slot):
        def sub(s, _):
            m = 4 * blk
            rhs = jnp.concatenate(
                [qb_s[slot, pl.ds(pl.multiple_of(s * m + i * blk, blk), blk), :] for i in range(4)], axis=1)
            y = dot(pq_s[...], rhs)
            k0 = pl.multiple_of(c * cq + s * 4 * kq, 4 * kq)
            for h in range(heads):
                for p in range(2):
                    pair = [y[h * kq:(h + 1) * kq, (2 * p + e) * hd:(2 * p + e + 1) * hd] for e in range(2)]
                    w_s[pl.ds(k0 + 2 * kq * p, 2 * kq), h * hd:(h + 1) * hd] = jnp.concatenate(pair, axis=0).astype(BF16)
            return 0
        for s in range(cq // (4 * kq)):
            sub(s, 0)

    def kv_body(c, slot):
        def sub(s, _):
            m = 2 * blk
            rhs = jnp.concatenate(
                [kvb_s[slot, k, pl.ds(pl.multiple_of(s * m + i * blk, blk), blk), :] for k in range(2) for i in range(2)], axis=1)
            y = dot(pk_s[...], rhs)
            k0 = pl.multiple_of(c * ck + s * 2 * kk, 2 * kk)
            for k in range(2):
                for i in range(2):
                    for h in range(kvh):
                        col = heads * hd + (k * kvh + h) * hd
                        w_s[pl.ds(k0 + i * kk, kk), col:col + hd] = y[h * kk:(h + 1) * kk, (2 * k + i) * hd:(2 * k + i + 1) * hd].astype(BF16)
            return 0
        for s in range(ck // (2 * kk)):
            sub(s, 0)

    run_kv = ring(dm // ck, kvb_s.shape[0], kv_copies, kv_body)
    run_q = ring(dm // cq, qb_s.shape[0], q_copies, q_body)

    bar = pltpu.get_barrier_semaphore()
    for d in range(1, n):
        pl.semaphore_signal(bar, inc=1, device_id={"sp": lax.rem(me + d, n)}, device_id_type=MESH)
    own = pltpu.make_async_copy(x_hbm.at[pl.ds(me * nb, nb)], x_s.at[:, pl.ds(pl.multiple_of(me * tl, tl), tl), :], lsem)
    own.start()
    r_i = lax.broadcasted_iota(jnp.int32, (blk, blk), 0)
    c_i = lax.broadcasted_iota(jnp.int32, (blk, blk), 1)
    pq_s[...] = jnp.where(c_i == (r_i % kq) * heads + r_i // kq, 1.0, 0.0).astype(BF16)
    pk_s[...] = jnp.where(c_i == (r_i % kk) * kvh + r_i // kk, 1.0, 0.0).astype(BF16)
    pl.semaphore_wait(bar, n - 1)
    sends = []
    half = n // 2
    for d in [half] + [v for k in range(half - 1, 0, -1) for v in (k, n - k)]:
        peer = lax.rem(me + d, n)
        cp = pltpu.make_async_remote_copy(
            src_ref=x_hbm.at[pl.ds(peer * nb, nb)], dst_ref=x_s.at[:, pl.ds(pl.multiple_of(me * tl, tl), tl), :],
            send_sem=ssem.at[d], recv_sem=rsem.at[d], device_id={"sp": peer}, device_id_type=MESH)
        cp.start()
        sends.append(cp)

    run_kv()
    run_q()
    slots_o = wo_s.shape[0]
    n_o = wo_hbm.shape[0] // tile
    for c in range(slots_o):
        for cp in o_copies(c, c):
            cp.start()
    own.wait()
    for cp in sends:
        cp.wait()

    for b in range(nb):
        xb = x_s[b]
        a_s[b * seq:(b + 1) * seq, :] = rms_rows(xb, g_ref[...]).astype(BF16)
        acc_s[b * seq:(b + 1) * seq, :] = xb.astype(F32)

    def kv_proj(c, _):
        col = pl.multiple_of(heads * hd + c * tile, tile)
        val = dot(a_s[...], w_s[:, pl.ds(col, tile)]).astype(BF16)
        for h in range(grp):
            kv_s[c * grp + h] = val[:, h * hd:(h + 1) * hd]
        return 0
    lax.fori_loop(0, 2 * kvh // grp, kv_proj, 0)

    q_s[0] = dot(a_s[...], w_s[:, 0:tile]).astype(BF16)
    row_t = lax.broadcasted_iota(jnp.int32, (grp * seq, seq), 0) % seq
    col_t = lax.broadcasted_iota(jnp.int32, (grp * seq, seq), 1)
    causal = row_t >= col_t

    def group(j, _):
        slot = lax.rem(j, slots_o)
        nxt = jnp.minimum(j + 1, n_o - 1)
        cur = lax.rem(j, 2)
        q_next = dot(a_s[...], w_s[:, pl.ds(pl.multiple_of(nxt * tile, tile), tile)]).astype(BF16)
        outs = []
        for b in range(nb):
            qb = q_s[cur, b * seq:(b + 1) * seq, :]
            q4 = jnp.concatenate([qb[:, g * hd:(g + 1) * hd] for g in range(grp)], axis=0)
            kb = kv_s[j, b * seq:(b + 1) * seq, :]
            vb = kv_s[kvh + j, b * seq:(b + 1) * seq, :]
            s = dot_nt(q4, kb) * (hd ** -0.5)
            s = jnp.where(causal, s, -jnp.inf)
            e = jnp.exp(s - jnp.max(s, axis=-1, keepdims=True))
            p = (e / jnp.sum(e, axis=-1, keepdims=True)).astype(BF16)
            o = dot(p, vb).astype(BF16)
            outs.append(jnp.concatenate([o[g * seq:(g + 1) * seq, :] for g in range(grp)], axis=1))
        q_s[1 - cur] = q_next
        for cp in o_copies(j, slot):
            cp.wait()
        acc_s[...] += dot(jnp.concatenate(outs, axis=0), wo_s[slot])

        @pl.when(j + slots_o < n_o)
        def _():
            for cp in o_copies(j + slots_o, slot):
                cp.start()
        return 0
    lax.fori_loop(0, n_o, group, 0)
    h_ref[...] = acc_s[...].astype(BF16)


def head(x, g, wq, wk, wv, wo, n):
    batch, tl, dm = x.shape
    heads, hd = wq.shape[1:]
    kvh = wk.shape[1]
    nb, seq = batch // n, tl * n
    rows = nb * seq
    grp = heads // kvh
    tile = grp * hd
    blk = 256
    cq, ck, slots_q, slots_o = 128, 320, 3, 3
    any_ = pl.BlockSpec(memory_space=pl.ANY)
    vm = pl.BlockSpec(memory_space=pltpu.VMEM)
    flat = lambda w: w.reshape(-1, w.shape[-1])
    return pl.pallas_call(
        functools.partial(head_kernel, n, heads, kvh, hd),
        out_shape=jax.ShapeDtypeStruct((rows, dm), BF16),
        in_specs=[any_, vm, any_, any_, any_, any_],
        out_specs=vm,
        scratch_shapes=[
            pltpu.VMEM((nb, seq, dm), BF16),
            pltpu.VMEM((dm, (heads + 2 * kvh) * hd), BF16),
            pltpu.VMEM((slots_q, cq * heads, hd), BF16),
            pltpu.VMEM((2, 2, ck * kvh, hd), BF16),
            pltpu.VMEM((slots_o, tile, dm), BF16),
            pltpu.VMEM((rows, dm), BF16),
            pltpu.VMEM((2 * kvh, rows, hd), BF16),
            pltpu.VMEM((2, rows, tile), BF16),
            pltpu.VMEM((rows, dm), F32),
            pltpu.VMEM((blk, blk), BF16),
            pltpu.VMEM((blk, blk), BF16),
            pltpu.SemaphoreType.DMA((n,)),
            pltpu.SemaphoreType.DMA((n,)),
            pltpu.SemaphoreType.DMA,
            pltpu.SemaphoreType.DMA((slots_q,)),
            pltpu.SemaphoreType.DMA((2, 2)),
            pltpu.SemaphoreType.DMA((slots_o,)),
        ],
        compiler_params=pltpu.CompilerParams(collective_id=0, has_side_effects=True, vmem_limit_bytes=63 << 20),
        name="head",
    )(x, g, flat(wq), flat(wk), flat(wv), flat(wo))


def zero_of(vals):
    return jnp.maximum(functools.reduce(jnp.minimum, vals, jnp.zeros_like(vals[0])), 0.0)


def tail_kernel(n, seq, dt_rank, n_state, h_ref, mg_ref, wg_hbm, wu_hbm, wd_hbm, ug_ref, wx_hbm, cw_ref, cb_ref, wxp_hbm,
                dtn_ref, bn_ref, cn_ref, wdt_hbm, dtb_ref, alog_ref, dsk_ref, wz_hbm, wo_hbm, o_hbm,
                w_s, d_s, u_s, acc_s, act_s, c_s, xi_s, r_s, dt_s, b_s, cc_s, dl_s, dx_s, y_s, a_s, st_s, z_s, gate_s, o_s,
                wxp_s, wdt_s, wsem, dsem, psem, ssem, rsem, lsem):
    me = lax.axis_index("sp")
    rows, dm = acc_s.shape
    slots, _, _, half_w = w_s.shape
    slots_d = d_s.shape[0]
    tile = 2 * half_w
    ne, nf = wx_hbm.shape[1] // tile, wg_hbm.shape[1] // half_w
    sub = tile // 128
    nb, tl = rows // seq, seq // n
    part = 256
    n_part = tile // part
    per = half_w // part
    tc = seq // n_part

    bar = pltpu.get_barrier_semaphore()
    for d in range(1, n):
        pl.semaphore_signal(bar, inc=1, device_id={"sp": lax.rem(me + d, n)}, device_id_type=MESH)

    def w_pair(k, a, b, ka, kb):
        slot = lax.rem(k, slots)
        return [pltpu.make_async_copy(w.at[:, pl.ds(pl.multiple_of(q * half_w, half_w), half_w)], w_s.at[slot, r], wsem.at[slot, r])
                for r, (w, q) in enumerate(((a, ka), (b, kb)))]

    def w_start(k):
        @pl.when(k < nf)
        def _():
            for cp in w_pair(k, wg_hbm, wu_hbm, k, k):
                cp.start()

        @pl.when((k >= nf) & (k < nf + ne))
        def _():
            for cp in w_pair(k, wx_hbm, wx_hbm, 2 * (k - nf), 2 * (k - nf) + 1):
                cp.start()

        @pl.when((k >= nf + ne) & (k < nf + 2 * ne))
        def _():
            for cp in w_pair(k, wz_hbm, wz_hbm, 2 * (k - nf - ne), 2 * (k - nf - ne) + 1):
                cp.start()

    def w_wait(k):
        for cp in w_pair(k, wg_hbm, wu_hbm, 0, 0):
            cp.wait()

    def d_copy(k, w, q):
        slot = lax.rem(k, slots_d)
        return pltpu.make_async_copy(w.at[pl.ds(pl.multiple_of(q * half_w, half_w), half_w)], d_s.at[slot], dsem.at[slot])

    def d_start(k):
        @pl.when(k < nf)
        def _():
            d_copy(k, wd_hbm, k).start()

        @pl.when((k >= nf) & (k < nf + 2 * ne))
        def _():
            d_copy(k, wo_hbm, k - nf).start()

    def d_wait(k):
        d_copy(k, wd_hbm, 0).wait()

    for k in range(max(slots, slots_d)):
        if k < slots:
            w_start(k)
        if k < slots_d:
            d_start(k)
    small = [pltpu.make_async_copy(wxp_hbm, wxp_s, psem.at[0]), pltpu.make_async_copy(wdt_hbm, wdt_s, psem.at[1])]
    for cp in small:
        cp.start()

    u_s[0:rows, :] = rms_rows(h_ref[...], mg_ref[...]).astype(BF16)
    acc_s[...] = h_ref[...].astype(F32)
    w_wait(0)
    act_s[0] = (silu(dot(u_s[0:rows, :], w_s[0, 0])) * dot(u_s[0:rows, :], w_s[0, 1])).astype(BF16)
    w_start(slots)

    def ff(k, _):
        slot, prev = lax.rem(k, slots), lax.rem(k - 1, slots_d)
        w_wait(k)
        d_wait(k - 1)
        gate = dot(u_s[0:rows, :], w_s[slot, 0])
        up = dot(u_s[0:rows, :], w_s[slot, 1])
        acc_s[...] += dot(act_s[lax.rem(k + 1, 2)], d_s[prev])
        act_s[lax.rem(k, 2)] = (silu(gate) * up).astype(BF16)
        w_start(k + slots)
        d_start(k - 1 + slots_d)
        return 0
    lax.fori_loop(1, nf, ff, 0)
    d_wait(nf - 1)
    h2 = (acc_s[...] + dot(act_s[(nf - 1) % 2], d_s[(nf - 1) % slots_d])).astype(BF16)
    d_start(nf - 1 + slots_d)
    acc_s[...] = h2.astype(F32)
    u_s[0:rows, :] = rms_rows(acc_s[...], ug_ref[...]).astype(BF16)

    r_s[...] = jnp.zeros_like(r_s)
    gate_s[...] = jnp.zeros_like(gate_s)

    def in_proj(e):
        k = nf + e
        slot = lax.rem(k, slots)
        w_wait(k)
        for r in range(2):
            xi_s[lax.rem(e, 2), :, r * half_w:(r + 1) * half_w] = dot(u_s[0:rows, :], w_s[slot, r]).astype(BF16)

    def conv(e):
        col = pl.ds(pl.multiple_of(e * tile, tile), tile)
        xi = xi_s[lax.rem(e, 2)].astype(F32)
        t_idx = lax.broadcasted_iota(jnp.int32, xi.shape, 0) % seq
        acc = cb_ref[col].astype(F32).reshape(1, -1) + xi * cw_ref[CONV - 1:CONV, col].astype(F32)
        for s in range(1, CONV):
            prev = jnp.where(t_idx >= s, pltpu.roll(xi, s, 0), 0.0)
            acc = acc + prev * cw_ref[CONV - 1 - s:CONV - s, col].astype(F32)
        c = silu(acc).astype(BF16)
        c_s[e] = c
        r_s[...] += dot_nt(c, wxp_s[:, col])

    in_proj(0)
    w_start(nf + slots)
    for cp in small:
        cp.wait()

    def phase_a(e, _):
        in_proj(e)
        conv(e - 1)
        w_start(nf + e + slots)
        return 0
    lax.fori_loop(1, ne, phase_a, 0)

    kz = nf + ne
    w_wait(kz)
    for r in range(2):
        z_s[0, :, r * half_w:(r + 1) * half_w] = dot(u_s[0:rows, :], w_s[kz % slots, r]).astype(BF16)
    conv(ne - 1)
    w_start(kz + slots)

    r = r_s[...]
    dt_s[...] = rms_rows(r[:, :dt_rank], dtn_ref[...]).astype(BF16)
    bm = rms_rows(r[:, dt_rank:dt_rank + n_state], bn_ref[...])
    cm = rms_rows(r[:, dt_rank + n_state:], cn_ref[...])
    for k in range(n_state):
        b_s[k] = jnp.broadcast_to(bm[:, k:k + 1], (rows, 128))
        cc_s[k] = jnp.broadcast_to(cm[:, k:k + 1], (rows, 128))

    def phase_b(e, _):
        col = pl.ds(pl.multiple_of(e * tile, tile), tile)
        zc, zn = lax.rem(e, 2), lax.rem(e + 1, 2)
        z_tile, o_tile = jnp.minimum(e + 1, ne - 1), jnp.maximum(e - 1, 0)
        slot_z = lax.rem(kz + z_tile, slots)

        @pl.when(e + 1 < ne)
        def _():
            w_wait(kz + e + 1)

        @pl.when(e != 1)
        def _():
            for q in range(2):
                d_wait(nf + 2 * o_tile + q)

        delta = softplus(dot(dt_s[...], wdt_s[:, col]) + dtb_ref[:, col])
        dx = delta * c_s[e].astype(F32)
        a2 = -jnp.exp(alog_ref[:, col]) * LOG2E
        for j in range(sub):
            dl_s[pl.ds(j, rows, stride=sub), :] = delta[:, j * 128:(j + 1) * 128]
            dx_s[pl.ds(j, rows, stride=sub), :] = dx[:, j * 128:(j + 1) * 128]
            a_s[pl.ds(j, n_state, stride=sub), :] = a2[:, j * 128:(j + 1) * 128]
        st_s[...] = jnp.zeros_like(st_s)

        def chunk(c, _):
            spare = pl.multiple_of(rows + 16 * lax.div(c, n_part), 16)
            k0 = pl.multiple_of(c * part, part)
            kp = pl.multiple_of(lax.rem(c, per) * part, part)
            slot_o = lax.rem(nf + 2 * o_tile + c // per, slots_d)
            n_k = dm // 256
            places = [(p * (nb * tc - LAG)) // (2 * n_k) for p in range(2 * n_k)]
            lhs, after = [], {}

            def fence(ref, y):
                ref[pl.ds(spare, 16), 0:128] = jnp.concatenate([y, y], axis=0).astype(BF16)

            for b in range(nb):
                state = [st_s[b * n_state + k] for k in range(n_state)]
                for tt in range(tc):
                    step = b * tc + tt
                    tok = b * seq + c * tc + tt
                    row = pl.multiple_of(tok * sub, sub)
                    dl = dl_s[pl.ds(row, sub), :]
                    dxt = dx_s[pl.ds(row, sub), :]
                    if step in after:
                        dl = dl + after[step]
                    parts = [None] * 2
                    for k in range(n_state):
                        bb = b_s[k, pl.ds(tok, sub, stride=0), :]
                        ct = cc_s[k, pl.ds(tok, sub, stride=0), :]
                        s = jnp.exp2(dl * a_s[k * sub:(k + 1) * sub, :]) * state[k] + dxt * bb
                        state[k] = s
                        term = s * ct
                        parts[k % 2] = term if parts[k % 2] is None else parts[k % 2] + term
                    y = parts[0] + parts[1]
                    y_s[pl.ds(row, sub), :] = y
                    if step == tc - 1:
                        after[tc] = zero_of([y])
                    if step in places:
                        p = places.index(step)
                        q = p // 2
                        if p % 2 == 0:
                            fence(u_s, y)
                            lhs.append(u_s[0:rows, q * 256:(q + 1) * 256])
                        else:
                            fence(gate_s, y)
                            lanes = slice(q * 256, (q + 1) * 256)
                            ov = dot(gate_s[0:rows, pl.ds(k0, part)], d_s[slot_o, pl.ds(kp, part), lanes])
                            acc_s[:, lanes] += ov
                            after[step + LAG] = zero_of([ov[rows - 8:, l0:l0 + 128] for l0 in (0, 128)])
                        if p == 2 * n_k - 2:
                            zv = dot(jnp.concatenate(lhs, axis=1), w_s[slot_z, c // per, :, pl.ds(kp, part)])
                            z_s[zn, :, pl.ds(k0, part)] = zv.astype(BF16)
                            after[step + LAG] = zero_of([zv[r0:r0 + 8, l0:l0 + 128] for r0 in (0, rows - 8) for l0 in (0, part - 128)])
                for k in range(n_state):
                    st_s[b * n_state + k] = state[k]
            return 0

        lax.fori_loop(0, n_part, chunk, 0)
        w_start(kz + e + 1 + slots)

        @pl.when(e >= 1)
        def _():
            for q in range(2):
                d_start(nf + 2 * (e - 1) + q + slots_d)

        for j in range(sub):
            lanes = slice(j * 128, (j + 1) * 128)
            dlanes = pl.ds(pl.multiple_of(e * tile + j * 128, 128), 128)
            y = y_s[pl.ds(j, rows, stride=sub), :] + dsk_ref[:, dlanes] * c_s[e, :, lanes].astype(F32)
            gate_s[0:rows, lanes] = (y * silu(z_s[zc, :, lanes].astype(F32))).astype(BF16)
        return 0
    lax.fori_loop(0, ne, phase_b, 0)

    n_out, _, _, w = o_s.shape
    pl.semaphore_wait(bar, n - 1)
    half = n // 2
    order = [half] + [v for k in range(half - 1, 0, -1) for v in (k, n - k)]
    copies = []

    def send(q):
        lanes = slice(q * w, (q + 1) * w)
        for d in order:
            peer = lax.rem(me + d, n)
            cp = pltpu.make_async_remote_copy(
                src_ref=o_s.at[q, :, pl.ds(pl.multiple_of(peer * tl, tl), tl), :],
                dst_ref=o_hbm.at[pl.ds(me * nb, nb), :, lanes],
                send_sem=ssem.at[q, d], recv_sem=rsem.at[q, d], device_id={"sp": peer}, device_id_type=MESH)
            cp.start()
            copies.append(cp)
        cp = pltpu.make_async_copy(o_s.at[q, :, pl.ds(pl.multiple_of(me * tl, tl), tl), :],
                                   o_hbm.at[pl.ds(me * nb, nb), :, lanes], lsem.at[q])
        cp.start()
        copies.append(cp)

    for q in range(2):
        d_wait(nf + 2 * (ne - 1) + q)
    s0, s1 = [(nf + 2 * (ne - 1) + q) % slots_d for q in range(2)]
    for q in range(n_out):
        lanes = slice(q * w, (q + 1) * w)
        val = acc_s[:, lanes] + dot(gate_s[0:rows, :half_w], d_s[s0, :, lanes]) + dot(gate_s[0:rows, half_w:], d_s[s1, :, lanes])
        for b in range(nb):
            o_s[q, b] = val[b * seq:(b + 1) * seq, :].astype(BF16)
        if q:
            send(q - 1)
    send(n_out - 1)
    for cp in copies:
        cp.wait()


def tail(h, mg, wg, wu, wd, ug, wx, wz, cw, cb, wxp_t, dtn, bn, cn, wdt, dtb, alog_t, dsk, wo, seq, n, half_w=512, n_out=5, slots=3, slots_d=4):
    rows, dm = h.shape
    inner = wx.shape[1]
    dt_rank, n_state = wdt.shape[0], alog_t.shape[0]
    nr = wxp_t.shape[0]
    tile = 2 * half_w
    ne = inner // tile
    sub = tile // 128
    nb, tl = rows // seq, seq // n
    any_ = pl.BlockSpec(memory_space=pl.ANY)
    vm = pl.BlockSpec(memory_space=pltpu.VMEM)
    return pl.pallas_call(
        functools.partial(tail_kernel, n, seq, dt_rank, n_state),
        out_shape=jax.ShapeDtypeStruct((nb * n, tl, dm), BF16),
        in_specs=[vm, vm, any_, any_, any_, vm, any_, vm, vm, any_, vm, vm, vm, any_, vm, vm, vm, any_, any_],
        out_specs=any_,
        scratch_shapes=[
            pltpu.VMEM((slots, 2, dm, half_w), BF16),
            pltpu.VMEM((slots_d, half_w, dm), BF16),
            pltpu.VMEM((rows + 16, dm), BF16),
            pltpu.VMEM((rows, dm), F32),
            pltpu.VMEM((2, rows, half_w), BF16),
            pltpu.VMEM((ne, rows, tile), BF16),
            pltpu.VMEM((2, rows, tile), BF16),
            pltpu.VMEM((rows, nr), F32),
            pltpu.VMEM((rows, dt_rank), BF16),
            pltpu.VMEM((n_state, rows, 128), F32),
            pltpu.VMEM((n_state, rows, 128), F32),
            pltpu.VMEM((rows * sub, 128), F32),
            pltpu.VMEM((rows * sub, 128), F32),
            pltpu.VMEM((rows * sub, 128), F32),
            pltpu.VMEM((n_state * sub, 128), F32),
            pltpu.VMEM((nb * n_state, sub, 128), F32),
            pltpu.VMEM((2, rows, tile), BF16),
            pltpu.VMEM((rows + 16, tile), BF16),
            pltpu.VMEM((n_out, nb, seq, dm // n_out), BF16),
            pltpu.VMEM((nr, inner), BF16),
            pltpu.VMEM((dt_rank, inner), BF16),
            pltpu.SemaphoreType.DMA((slots, 2)),
            pltpu.SemaphoreType.DMA((slots_d,)),
            pltpu.SemaphoreType.DMA((2,)),
            pltpu.SemaphoreType.DMA((n_out, n)),
            pltpu.SemaphoreType.DMA((n_out, n)),
            pltpu.SemaphoreType.DMA((n_out,)),
        ],
        compiler_params=pltpu.CompilerParams(collective_id=1, has_side_effects=True, vmem_limit_bytes=55 << 20),
        name="tail",
    )(h, mg, wg, wu, wd, ug, wx, cw, cb, wxp_t, dtn, bn, cn, wdt, dtb, alog_t, dsk, wz, wo)


def layer_pair(hidden, attn_norm, w_q, w_k, w_v, w_o, mlp_norm, w_gate, w_up, w_down, mamba_norm, w_in_x, w_in_z, conv_w, conv_b, w_xproj, dt_norm, b_norm, c_norm, w_dt, dt_bias, a_log, d_skip, w_out, n_shards):
    batch, tl, dm = hidden.shape
    seq = tl * n_shards
    row = lambda v: v.reshape(1, -1)
    h = head(hidden, attn_norm, w_q, w_k, w_v, w_o, n_shards)
    return tail(h, mlp_norm, w_gate, w_up, w_down, mamba_norm, w_in_x, w_in_z, conv_w, conv_b, w_xproj.T, row(dt_norm), row(b_norm), row(c_norm), w_dt, row(dt_bias), a_log.T, row(d_skip), w_out, seq, n_shards)


def solution(mesh):
    act_spec = P("dp", "sp", None)
    return jax.shard_map(
        functools.partial(layer_pair, n_shards=mesh.shape["sp"]),
        mesh=mesh,
        in_specs=(act_spec,) + (P(),) * 23,
        out_specs=act_spec,
        check_vma=False,
    )
```

```python
import functools
import math

import jax
import jax.numpy as jnp
from jax import lax
from jax.experimental import pallas as pl
from jax.experimental.pallas import tpu as pltpu
from jax.sharding import PartitionSpec as P

EPS = 1e-6
CONV = 4
LAG = 20
F32 = jnp.float32
BF16 = jnp.bfloat16
MESH = pl.DeviceIdType.MESH
LOG2E = 1.0 / math.log(2.0)


def dot(a, b):
    return jnp.dot(a, b, preferred_element_type=F32)


def dot_nt(a, b):
    return lax.dot_general(a, b, (((1,), (1,)), ((), ())), preferred_element_type=F32)


def rms_rows(v, gain):
    v = v.astype(F32)
    inv = lax.rsqrt(jnp.mean(v * v, axis=-1, keepdims=True) + EPS)
    return v * inv * gain.astype(F32).reshape(1, -1)


def silu(v):
    return v / (1.0 + jnp.exp(-v))


def softplus(v):
    w = jnp.exp(-jnp.abs(v))
    u = 1.0 + w
    return jnp.maximum(v, 0.0) + (jnp.log(u) + (w - (u - 1.0)))


def ring(n, slots, copies, body):
    for c in range(min(slots, n)):
        for cp in copies(c, c):
            cp.start()

    def run():
        def step(c, _):
            slot = lax.rem(c, slots)
            for cp in copies(c, slot):
                cp.wait()
            body(c, slot)

            @pl.when(c + slots < n)
            def _():
                for cp in copies(c + slots, slot):
                    cp.start()
            return 0
        lax.fori_loop(0, n, step, 0)
    return run


def head_kernel(n, heads, kvh, hd, x_hbm, g_ref, wq_hbm, wk_hbm, wv_hbm, wo_hbm, h_ref,
                x_s, w_s, qb_s, kvb_s, wo_s, a_s, kv_s, q_s, o_s, acc_s, pq_s, pk_s,
                ssem, rsem, lsem, qsem, kvsem, osem):
    me = lax.axis_index("sp")
    nb, seq, dm = x_s.shape
    tl = seq // n
    rows = nb * seq
    grp = heads // kvh
    tile = grp * hd
    blk = pq_s.shape[0]
    kq, kk = blk // heads, blk // kvh
    cq, ck = qb_s.shape[1] // heads, kvb_s.shape[2] // kvh

    def q_copies(c, slot):
        m = cq * heads
        return [pltpu.make_async_copy(wq_hbm.at[pl.ds(pl.multiple_of(c * m, m), m)], qb_s.at[slot], qsem.at[slot])]

    def kv_copies(c, slot):
        m = ck * kvh
        return [pltpu.make_async_copy(w.at[pl.ds(pl.multiple_of(c * m, m), m)], kvb_s.at[slot, k], kvsem.at[slot, k])
                for k, w in enumerate((wk_hbm, wv_hbm))]

    def o_copies(c, slot):
        return [pltpu.make_async_copy(wo_hbm.at[pl.ds(pl.multiple_of(c * tile, tile), tile)], wo_s.at[slot], osem.at[slot])]

    def q_body(c, slot):
        def sub(s, _):
            m = 4 * blk
            rhs = jnp.concatenate(
                [qb_s[slot, pl.ds(pl.multiple_of(s * m + i * blk, blk), blk), :] for i in range(4)], axis=1)
            y = dot(pq_s[...], rhs)
            k0 = pl.multiple_of(c * cq + s * 4 * kq, 4 * kq)
            for h in range(heads):
                for p in range(2):
                    pair = [y[h * kq:(h + 1) * kq, (2 * p + e) * hd:(2 * p + e + 1) * hd] for e in range(2)]
                    w_s[pl.ds(k0 + 2 * kq * p, 2 * kq), h * hd:(h + 1) * hd] = jnp.concatenate(pair, axis=0).astype(BF16)
            return 0
        for s in range(cq // (4 * kq)):
            sub(s, 0)

    def kv_body(c, slot):
        def sub(s, _):
            m = 2 * blk
            rhs = jnp.concatenate(
                [kvb_s[slot, k, pl.ds(pl.multiple_of(s * m + i * blk, blk), blk), :] for k in range(2) for i in range(2)], axis=1)
            y = dot(pk_s[...], rhs)
            k0 = pl.multiple_of(c * ck + s * 2 * kk, 2 * kk)
            for k in range(2):
                for i in range(2):
                    for h in range(kvh):
                        col = heads * hd + (k * kvh + h) * hd
                        w_s[pl.ds(k0 + i * kk, kk), col:col + hd] = y[h * kk:(h + 1) * kk, (2 * k + i) * hd:(2 * k + i + 1) * hd].astype(BF16)
            return 0
        for s in range(ck // (2 * kk)):
            sub(s, 0)

    run_kv = ring(dm // ck, kvb_s.shape[0], kv_copies, kv_body)
    run_q = ring(dm // cq, qb_s.shape[0], q_copies, q_body)

    bar = pltpu.get_barrier_semaphore()
    for d in range(1, n):
        pl.semaphore_signal(bar, inc=1, device_id={"sp": lax.rem(me + d, n)}, device_id_type=MESH)
    own = pltpu.make_async_copy(x_hbm.at[pl.ds(me * nb, nb)], x_s.at[:, pl.ds(pl.multiple_of(me * tl, tl), tl), :], lsem)
    own.start()
    r_i = lax.broadcasted_iota(jnp.int32, (blk, blk), 0)
    c_i = lax.broadcasted_iota(jnp.int32, (blk, blk), 1)
    pq_s[...] = jnp.where(c_i == (r_i % kq) * heads + r_i // kq, 1.0, 0.0).astype(BF16)
    pk_s[...] = jnp.where(c_i == (r_i % kk) * kvh + r_i // kk, 1.0, 0.0).astype(BF16)
    pl.semaphore_wait(bar, n - 1)
    sends = []
    half = n // 2
    for d in [half] + [v for k in range(half - 1, 0, -1) for v in (k, n - k)]:
        peer = lax.rem(me + d, n)
        cp = pltpu.make_async_remote_copy(
            src_ref=x_hbm.at[pl.ds(peer * nb, nb)], dst_ref=x_s.at[:, pl.ds(pl.multiple_of(me * tl, tl), tl), :],
            send_sem=ssem.at[d], recv_sem=rsem.at[d], device_id={"sp": peer}, device_id_type=MESH)
        cp.start()
        sends.append(cp)

    run_kv()
    run_q()
    slots_o = wo_s.shape[0]
    n_o = wo_hbm.shape[0] // tile
    for c in range(slots_o):
        for cp in o_copies(c, c):
            cp.start()
    own.wait()
    for cp in sends:
        cp.wait()

    for b in range(nb):
        xb = x_s[b]
        a_s[b * seq:(b + 1) * seq, :] = rms_rows(xb, g_ref[...]).astype(BF16)
        acc_s[b * seq:(b + 1) * seq, :] = xb.astype(F32)

    def kv_proj(c, _):
        col = pl.multiple_of(heads * hd + c * tile, tile)
        val = dot(a_s[...], w_s[:, pl.ds(col, tile)]).astype(BF16)
        for h in range(grp):
            kv_s[c * grp + h] = val[:, h * hd:(h + 1) * hd]
        return 0
    lax.fori_loop(0, 2 * kvh // grp, kv_proj, 0, unroll=True)

    q_s[0] = dot(a_s[...], w_s[:, 0:tile]).astype(BF16)
    o_s[1] = jnp.zeros_like(o_s[1])
    row_t = lax.broadcasted_iota(jnp.int32, (grp * seq, seq), 0) % seq
    col_t = lax.broadcasted_iota(jnp.int32, (grp * seq, seq), 1)
    causal = row_t >= col_t

    def group(j, _):
        done = jnp.maximum(j - 1, 0)
        slot = lax.rem(done, slots_o)
        nxt = jnp.minimum(j + 1, n_o - 1)
        cur = lax.rem(j, 2)

        @pl.when(j != 1)
        def _():
            for cp in o_copies(done, slot):
                cp.wait()

        scores = []
        for b in range(nb):
            qb = q_s[cur, b * seq:(b + 1) * seq, :]
            q4 = jnp.concatenate([qb[:, g * hd:(g + 1) * hd] for g in range(grp)], axis=0)
            scores.append(dot_nt(q4, kv_s[j, b * seq:(b + 1) * seq, :]))
        q_next = dot(a_s[...], w_s[:, pl.ds(pl.multiple_of(nxt * tile, tile), tile)]).astype(BF16)
        probs = []
        for s in scores:
            s = jnp.where(causal, s * (hd ** -0.5), -jnp.inf)
            e = jnp.exp(s - jnp.max(s, axis=-1, keepdims=True))
            probs.append((e / jnp.sum(e, axis=-1, keepdims=True)).astype(BF16))
        acc_s[...] += dot(o_s[1 - cur], wo_s[slot])
        for b in range(nb):
            o = dot(probs[b], kv_s[kvh + j, b * seq:(b + 1) * seq, :]).astype(BF16)
            for g in range(grp):
                o_s[cur, b * seq:(b + 1) * seq, g * hd:(g + 1) * hd] = o[g * seq:(g + 1) * seq, :]
        q_s[1 - cur] = q_next

        @pl.when((j >= 1) & (j - 1 + slots_o < n_o))
        def _():
            for cp in o_copies(j - 1 + slots_o, slot):
                cp.start()
        return 0
    lax.fori_loop(0, n_o, group, 0)
    last = (n_o - 1) % slots_o
    for cp in o_copies(n_o - 1, last):
        cp.wait()
    h_ref[...] = (acc_s[...] + dot(o_s[(n_o - 1) % 2], wo_s[last])).astype(BF16)


def head(x, g, wq, wk, wv, wo, n):
    batch, tl, dm = x.shape
    heads, hd = wq.shape[1:]
    kvh = wk.shape[1]
    nb, seq = batch // n, tl * n
    rows = nb * seq
    grp = heads // kvh
    tile = grp * hd
    blk = 256
    cq, ck, slots_q, slots_o = 128, 320, 3, 3
    any_ = pl.BlockSpec(memory_space=pl.ANY)
    vm = pl.BlockSpec(memory_space=pltpu.VMEM)
    flat = lambda w: w.reshape(-1, w.shape[-1])
    return pl.pallas_call(
        functools.partial(head_kernel, n, heads, kvh, hd),
        out_shape=jax.ShapeDtypeStruct((rows, dm), BF16),
        in_specs=[any_, vm, any_, any_, any_, any_],
        out_specs=vm,
        scratch_shapes=[
            pltpu.VMEM((nb, seq, dm), BF16),
            pltpu.VMEM((dm, (heads + 2 * kvh) * hd), BF16),
            pltpu.VMEM((slots_q, cq * heads, hd), BF16),
            pltpu.VMEM((2, 2, ck * kvh, hd), BF16),
            pltpu.VMEM((slots_o, tile, dm), BF16),
            pltpu.VMEM((rows, dm), BF16),
            pltpu.VMEM((2 * kvh, rows, hd), BF16),
            pltpu.VMEM((2, rows, tile), BF16),
            pltpu.VMEM((2, rows, tile), BF16),
            pltpu.VMEM((rows, dm), F32),
            pltpu.VMEM((blk, blk), BF16),
            pltpu.VMEM((blk, blk), BF16),
            pltpu.SemaphoreType.DMA((n,)),
            pltpu.SemaphoreType.DMA((n,)),
            pltpu.SemaphoreType.DMA,
            pltpu.SemaphoreType.DMA((slots_q,)),
            pltpu.SemaphoreType.DMA((2, 2)),
            pltpu.SemaphoreType.DMA((slots_o,)),
        ],
        compiler_params=pltpu.CompilerParams(collective_id=0, has_side_effects=True, vmem_limit_bytes=63 << 20),
        name="head",
    )(x, g, flat(wq), flat(wk), flat(wv), flat(wo))


def zero_of(vals):
    return jnp.maximum(functools.reduce(jnp.minimum, vals, jnp.zeros_like(vals[0])), 0.0)


def tail_kernel(n, seq, dt_rank, n_state, h_ref, mg_ref, wg_hbm, wu_hbm, wd_hbm, ug_ref, wx_hbm, cw_ref, cb_ref, wxp_hbm,
                dtn_ref, bn_ref, cn_ref, wdt_hbm, dtb_ref, alog_ref, dsk_ref, wz_hbm, wo_hbm, o_hbm,
                w_s, d_s, u_s, acc_s, act_s, c_s, xi_s, r_s, dt_s, b_s, cc_s, dl_s, dx_s, y_s, a_s, st_s, z_s, gate_s, o_s,
                wxp_s, wdt_s, wsem, dsem, psem, ssem, rsem, lsem):
    me = lax.axis_index("sp")
    rows, dm = acc_s.shape
    slots, _, _, half_w = w_s.shape
    slots_d = d_s.shape[0]
    tile = 2 * half_w
    ne, nf = wx_hbm.shape[1] // tile, wg_hbm.shape[1] // half_w
    sub = tile // 128
    nb, tl = rows // seq, seq // n
    part = 256
    n_part = tile // part
    per = half_w // part
    tc = seq // n_part

    bar = pltpu.get_barrier_semaphore()
    for d in range(1, n):
        pl.semaphore_signal(bar, inc=1, device_id={"sp": lax.rem(me + d, n)}, device_id_type=MESH)

    def w_pair(k, a, b, ka, kb):
        slot = lax.rem(k, slots)
        return [pltpu.make_async_copy(w.at[:, pl.ds(pl.multiple_of(q * half_w, half_w), half_w)], w_s.at[slot, r], wsem.at[slot, r])
                for r, (w, q) in enumerate(((a, ka), (b, kb)))]

    def w_start(k):
        @pl.when(k < nf)
        def _():
            for cp in w_pair(k, wg_hbm, wu_hbm, k, k):
                cp.start()

        @pl.when((k >= nf) & (k < nf + ne))
        def _():
            for cp in w_pair(k, wx_hbm, wx_hbm, 2 * (k - nf), 2 * (k - nf) + 1):
                cp.start()

        @pl.when((k >= nf + ne) & (k < nf + 2 * ne))
        def _():
            for cp in w_pair(k, wz_hbm, wz_hbm, 2 * (k - nf - ne), 2 * (k - nf - ne) + 1):
                cp.start()

    def w_wait(k):
        for cp in w_pair(k, wg_hbm, wu_hbm, 0, 0):
            cp.wait()

    def d_copy(k, w, q):
        slot = lax.rem(k, slots_d)
        return pltpu.make_async_copy(w.at[pl.ds(pl.multiple_of(q * half_w, half_w), half_w)], d_s.at[slot], dsem.at[slot])

    def d_start(k):
        @pl.when(k < nf)
        def _():
            d_copy(k, wd_hbm, k).start()

        @pl.when((k >= nf) & (k < nf + 2 * ne))
        def _():
            d_copy(k, wo_hbm, k - nf).start()

    def d_wait(k):
        d_copy(k, wd_hbm, 0).wait()

    for k in range(max(slots, slots_d)):
        if k < slots:
            w_start(k)
        if k < slots_d:
            d_start(k)
    small = [pltpu.make_async_copy(wxp_hbm, wxp_s, psem.at[0]), pltpu.make_async_copy(wdt_hbm, wdt_s, psem.at[1])]
    for cp in small:
        cp.start()

    u_s[0:rows, :] = rms_rows(h_ref[...], mg_ref[...]).astype(BF16)
    acc_s[...] = h_ref[...].astype(F32)
    w_wait(0)
    act_s[0] = (silu(dot(u_s[0:rows, :], w_s[0, 0])) * dot(u_s[0:rows, :], w_s[0, 1])).astype(BF16)
    w_start(slots)

    def ff(k, _):
        slot, prev = lax.rem(k, slots), lax.rem(k - 1, slots_d)
        w_wait(k)
        d_wait(k - 1)
        gate = dot(u_s[0:rows, :], w_s[slot, 0])
        up = dot(u_s[0:rows, :], w_s[slot, 1])
        acc_s[...] += dot(act_s[lax.rem(k + 1, 2)], d_s[prev])
        act_s[lax.rem(k, 2)] = (silu(gate) * up).astype(BF16)
        w_start(k + slots)
        d_start(k - 1 + slots_d)
        return 0
    lax.fori_loop(1, nf, ff, 0)
    d_wait(nf - 1)
    h2 = (acc_s[...] + dot(act_s[(nf - 1) % 2], d_s[(nf - 1) % slots_d])).astype(BF16)
    d_start(nf - 1 + slots_d)
    acc_s[...] = h2.astype(F32)
    u_s[0:rows, :] = rms_rows(acc_s[...], ug_ref[...]).astype(BF16)

    r_s[...] = jnp.zeros_like(r_s)
    gate_s[...] = jnp.zeros_like(gate_s)

    def in_proj(e):
        k = nf + e
        slot = lax.rem(k, slots)
        w_wait(k)
        for r in range(2):
            xi_s[lax.rem(e, 2), :, r * half_w:(r + 1) * half_w] = dot(u_s[0:rows, :], w_s[slot, r]).astype(BF16)

    def conv(e):
        col = pl.ds(pl.multiple_of(e * tile, tile), tile)
        xi = xi_s[lax.rem(e, 2)].astype(F32)
        t_idx = lax.broadcasted_iota(jnp.int32, xi.shape, 0) % seq
        acc = cb_ref[col].astype(F32).reshape(1, -1) + xi * cw_ref[CONV - 1:CONV, col].astype(F32)
        for s in range(1, CONV):
            prev = jnp.where(t_idx >= s, pltpu.roll(xi, s, 0), 0.0)
            acc = acc + prev * cw_ref[CONV - 1 - s:CONV - s, col].astype(F32)
        c = silu(acc).astype(BF16)
        c_s[e] = c
        r_s[...] += dot_nt(c, wxp_s[:, col])

    in_proj(0)
    w_start(nf + slots)
    for cp in small:
        cp.wait()

    def phase_a(e, _):
        in_proj(e)
        conv(e - 1)
        w_start(nf + e + slots)
        return 0
    lax.fori_loop(1, ne, phase_a, 0)

    kz = nf + ne
    w_wait(kz)
    for r in range(2):
        z_s[0, :, r * half_w:(r + 1) * half_w] = dot(u_s[0:rows, :], w_s[kz % slots, r]).astype(BF16)
    conv(ne - 1)
    w_start(kz + slots)

    r = r_s[...]
    dt_s[...] = rms_rows(r[:, :dt_rank], dtn_ref[...]).astype(BF16)
    bm = rms_rows(r[:, dt_rank:dt_rank + n_state], bn_ref[...])
    cm = rms_rows(r[:, dt_rank + n_state:], cn_ref[...])
    for k in range(n_state):
        b_s[k] = jnp.broadcast_to(bm[:, k:k + 1], (rows, 128))
        cc_s[k] = jnp.broadcast_to(cm[:, k:k + 1], (rows, 128))

    def phase_b(e, _):
        col = pl.ds(pl.multiple_of(e * tile, tile), tile)
        zc, zn = lax.rem(e, 2), lax.rem(e + 1, 2)
        z_tile, o_tile = jnp.minimum(e + 1, ne - 1), jnp.maximum(e - 1, 0)
        slot_z = lax.rem(kz + z_tile, slots)

        @pl.when(e + 1 < ne)
        def _():
            w_wait(kz + e + 1)

        @pl.when(e != 1)
        def _():
            for q in range(2):
                d_wait(nf + 2 * o_tile + q)

        delta = softplus(dot(dt_s[...], wdt_s[:, col]) + dtb_ref[:, col])
        dx = delta * c_s[e].astype(F32)
        a2 = -jnp.exp(alog_ref[:, col]) * LOG2E
        for j in range(sub):
            dl_s[pl.ds(j, rows, stride=sub), :] = delta[:, j * 128:(j + 1) * 128]
            dx_s[pl.ds(j, rows, stride=sub), :] = dx[:, j * 128:(j + 1) * 128]
            a_s[pl.ds(j, n_state, stride=sub), :] = a2[:, j * 128:(j + 1) * 128]
        st_s[...] = jnp.zeros_like(st_s)

        def chunk(c, _):
            spare = pl.multiple_of(rows + 16 * lax.div(c, n_part), 16)
            k0 = pl.multiple_of(c * part, part)
            kp = pl.multiple_of(lax.rem(c, per) * part, part)
            slot_o = lax.rem(nf + 2 * o_tile + c // per, slots_d)
            n_k = dm // 256
            places = [(p * (nb * tc - LAG)) // (2 * n_k) for p in range(2 * n_k)]
            lhs, after = [], {}

            def fence(ref, y):
                ref[pl.ds(spare, 16), 0:128] = jnp.concatenate([y, y], axis=0).astype(BF16)

            for b in range(nb):
                state = [st_s[b * n_state + k] for k in range(n_state)]
                for tt in range(tc):
                    step = b * tc + tt
                    tok = b * seq + c * tc + tt
                    row = pl.multiple_of(tok * sub, sub)
                    dl = dl_s[pl.ds(row, sub), :]
                    dxt = dx_s[pl.ds(row, sub), :]
                    if step in after:
                        dl = dl + after[step]
                    parts = [None] * 2
                    for k in range(n_state):
                        bb = b_s[k, pl.ds(tok, sub, stride=0), :]
                        ct = cc_s[k, pl.ds(tok, sub, stride=0), :]
                        s = jnp.exp2(dl * a_s[k * sub:(k + 1) * sub, :]) * state[k] + dxt * bb
                        state[k] = s
                        term = s * ct
                        parts[k % 2] = term if parts[k % 2] is None else parts[k % 2] + term
                    y = parts[0] + parts[1]
                    y_s[pl.ds(row, sub), :] = y
                    if step == tc - 1:
                        after[tc] = zero_of([y])
                    if step in places:
                        p = places.index(step)
                        q = p // 2
                        if p % 2 == 0:
                            fence(u_s, y)
                            lhs.append(u_s[0:rows, q * 256:(q + 1) * 256])
                        else:
                            fence(gate_s, y)
                            lanes = slice(q * 256, (q + 1) * 256)
                            ov = dot(gate_s[0:rows, pl.ds(k0, part)], d_s[slot_o, pl.ds(kp, part), lanes])
                            acc_s[:, lanes] += ov
                            after[step + LAG] = zero_of([ov[rows - 8:, l0:l0 + 128] for l0 in (0, 128)])
                        if p == 2 * n_k - 2:
                            zv = dot(jnp.concatenate(lhs, axis=1), w_s[slot_z, c // per, :, pl.ds(kp, part)])
                            z_s[zn, :, pl.ds(k0, part)] = zv.astype(BF16)
                            after[step + LAG] = zero_of([zv[r0:r0 + 8, l0:l0 + 128] for r0 in (0, rows - 8) for l0 in (0, part - 128)])
                for k in range(n_state):
                    st_s[b * n_state + k] = state[k]
            return 0

        lax.fori_loop(0, n_part, chunk, 0)
        w_start(kz + e + 1 + slots)

        @pl.when(e >= 1)
        def _():
            for q in range(2):
                d_start(nf + 2 * (e - 1) + q + slots_d)

        for j in range(sub):
            lanes = slice(j * 128, (j + 1) * 128)
            dlanes = pl.ds(pl.multiple_of(e * tile + j * 128, 128), 128)
            y = y_s[pl.ds(j, rows, stride=sub), :] + dsk_ref[:, dlanes] * c_s[e, :, lanes].astype(F32)
            gate_s[0:rows, lanes] = (y * silu(z_s[zc, :, lanes].astype(F32))).astype(BF16)
        return 0
    lax.fori_loop(0, ne, phase_b, 0)

    n_out, _, _, w = o_s.shape
    pl.semaphore_wait(bar, n - 1)
    half = n // 2
    order = [half] + [v for k in range(half - 1, 0, -1) for v in (k, n - k)]
    copies = []

    def send(q):
        lanes = slice(q * w, (q + 1) * w)
        for d in order:
            peer = lax.rem(me + d, n)
            cp = pltpu.make_async_remote_copy(
                src_ref=o_s.at[q, :, pl.ds(pl.multiple_of(peer * tl, tl), tl), :],
                dst_ref=o_hbm.at[pl.ds(me * nb, nb), :, lanes],
                send_sem=ssem.at[q, d], recv_sem=rsem.at[q, d], device_id={"sp": peer}, device_id_type=MESH)
            cp.start()
            copies.append(cp)
        cp = pltpu.make_async_copy(o_s.at[q, :, pl.ds(pl.multiple_of(me * tl, tl), tl), :],
                                   o_hbm.at[pl.ds(me * nb, nb), :, lanes], lsem.at[q])
        cp.start()
        copies.append(cp)

    for q in range(2):
        d_wait(nf + 2 * (ne - 1) + q)
    s0, s1 = [(nf + 2 * (ne - 1) + q) % slots_d for q in range(2)]
    for q in range(n_out):
        lanes = slice(q * w, (q + 1) * w)
        val = acc_s[:, lanes] + dot(gate_s[0:rows, :half_w], d_s[s0, :, lanes]) + dot(gate_s[0:rows, half_w:], d_s[s1, :, lanes])
        for b in range(nb):
            o_s[q, b] = val[b * seq:(b + 1) * seq, :].astype(BF16)
        if q:
            send(q - 1)
    send(n_out - 1)
    for cp in copies:
        cp.wait()


def tail(h, mg, wg, wu, wd, ug, wx, wz, cw, cb, wxp_t, dtn, bn, cn, wdt, dtb, alog_t, dsk, wo, seq, n, half_w=512, n_out=5, slots=3, slots_d=4):
    rows, dm = h.shape
    inner = wx.shape[1]
    dt_rank, n_state = wdt.shape[0], alog_t.shape[0]
    nr = wxp_t.shape[0]
    tile = 2 * half_w
    ne = inner // tile
    sub = tile // 128
    nb, tl = rows // seq, seq // n
    any_ = pl.BlockSpec(memory_space=pl.ANY)
    vm = pl.BlockSpec(memory_space=pltpu.VMEM)
    return pl.pallas_call(
        functools.partial(tail_kernel, n, seq, dt_rank, n_state),
        out_shape=jax.ShapeDtypeStruct((nb * n, tl, dm), BF16),
        in_specs=[vm, vm, any_, any_, any_, vm, any_, vm, vm, any_, vm, vm, vm, any_, vm, vm, vm, any_, any_],
        out_specs=any_,
        scratch_shapes=[
            pltpu.VMEM((slots, 2, dm, half_w), BF16),
            pltpu.VMEM((slots_d, half_w, dm), BF16),
            pltpu.VMEM((rows + 16, dm), BF16),
            pltpu.VMEM((rows, dm), F32),
            pltpu.VMEM((2, rows, half_w), BF16),
            pltpu.VMEM((ne, rows, tile), BF16),
            pltpu.VMEM((2, rows, tile), BF16),
            pltpu.VMEM((rows, nr), F32),
            pltpu.VMEM((rows, dt_rank), BF16),
            pltpu.VMEM((n_state, rows, 128), F32),
            pltpu.VMEM((n_state, rows, 128), F32),
            pltpu.VMEM((rows * sub, 128), F32),
            pltpu.VMEM((rows * sub, 128), F32),
            pltpu.VMEM((rows * sub, 128), F32),
            pltpu.VMEM((n_state * sub, 128), F32),
            pltpu.VMEM((nb * n_state, sub, 128), F32),
            pltpu.VMEM((2, rows, tile), BF16),
            pltpu.VMEM((rows + 16, tile), BF16),
            pltpu.VMEM((n_out, nb, seq, dm // n_out), BF16),
            pltpu.VMEM((nr, inner), BF16),
            pltpu.VMEM((dt_rank, inner), BF16),
            pltpu.SemaphoreType.DMA((slots, 2)),
            pltpu.SemaphoreType.DMA((slots_d,)),
            pltpu.SemaphoreType.DMA((2,)),
            pltpu.SemaphoreType.DMA((n_out, n)),
            pltpu.SemaphoreType.DMA((n_out, n)),
            pltpu.SemaphoreType.DMA((n_out,)),
        ],
        compiler_params=pltpu.CompilerParams(collective_id=1, has_side_effects=True, vmem_limit_bytes=55 << 20),
        name="tail",
    )(h, mg, wg, wu, wd, ug, wx, cw, cb, wxp_t, dtn, bn, cn, wdt, dtb, alog_t, dsk, wz, wo)


def layer_pair(hidden, attn_norm, w_q, w_k, w_v, w_o, mlp_norm, w_gate, w_up, w_down, mamba_norm, w_in_x, w_in_z, conv_w, conv_b, w_xproj, dt_norm, b_norm, c_norm, w_dt, dt_bias, a_log, d_skip, w_out, n_shards):
    batch, tl, dm = hidden.shape
    seq = tl * n_shards
    row = lambda v: v.reshape(1, -1)
    h = head(hidden, attn_norm, w_q, w_k, w_v, w_o, n_shards)
    return tail(h, mlp_norm, w_gate, w_up, w_down, mamba_norm, w_in_x, w_in_z, conv_w, conv_b, w_xproj.T, row(dt_norm), row(b_norm), row(c_norm), w_dt, row(dt_bias), a_log.T, row(d_skip), w_out, seq, n_shards)


def solution(mesh):
    act_spec = P("dp", "sp", None)
    return jax.shard_map(
        functools.partial(layer_pair, n_shards=mesh.shape["sp"]),
        mesh=mesh,
        in_specs=(act_spec,) + (P(),) * 23,
        out_specs=act_spec,
        check_vma=False,
    )
```

```python
import functools
import math

import jax
import jax.numpy as jnp
from jax import lax
from jax.experimental import pallas as pl
from jax.experimental.pallas import tpu as pltpu
from jax.sharding import PartitionSpec as P

EPS = 1e-6
CONV = 4
LAG = 20
F32 = jnp.float32
BF16 = jnp.bfloat16
MESH = pl.DeviceIdType.MESH
LOG2E = 1.0 / math.log(2.0)


def dot(a, b):
    return jnp.dot(a, b, preferred_element_type=F32)


def dot_nt(a, b):
    return lax.dot_general(a, b, (((1,), (1,)), ((), ())), preferred_element_type=F32)


def rms_rows(v, gain):
    v = v.astype(F32)
    inv = lax.rsqrt(jnp.mean(v * v, axis=-1, keepdims=True) + EPS)
    return v * inv * gain.astype(F32).reshape(1, -1)


def silu(v):
    return v / (1.0 + jnp.exp(-v))


def softplus(v):
    w = jnp.exp(-jnp.abs(v))
    u = 1.0 + w
    return jnp.maximum(v, 0.0) + (jnp.log(u) + (w - (u - 1.0)))


def ring(n, slots, copies, body):
    for c in range(min(slots, n)):
        for cp in copies(c, c):
            cp.start()

    def run():
        def step(c, _):
            slot = lax.rem(c, slots)
            for cp in copies(c, slot):
                cp.wait()
            body(c, slot)

            @pl.when(c + slots < n)
            def _():
                for cp in copies(c + slots, slot):
                    cp.start()
            return 0
        lax.fori_loop(0, n, step, 0)
    return run


def head_kernel(n, heads, kvh, hd, x_hbm, g_ref, wq_hbm, wk_hbm, wv_hbm, wo_hbm, h_ref,
                x_s, w_s, qb_s, kvb_s, wo_s, a_s, kv_s, q_s, o_s, acc_s, pq_s, pk_s,
                ssem, rsem, lsem, qsem, kvsem, osem):
    me = lax.axis_index("sp")
    nb, seq, dm = x_s.shape
    tl = seq // n
    rows = nb * seq
    grp = heads // kvh
    tile = grp * hd
    blk = pq_s.shape[0]
    kq, kk = blk // heads, blk // kvh
    cq, ck = qb_s.shape[1] // heads, kvb_s.shape[2] // kvh

    def q_copies(c, slot):
        m = cq * heads
        return [pltpu.make_async_copy(wq_hbm.at[pl.ds(pl.multiple_of(c * m, m), m)], qb_s.at[slot], qsem.at[slot])]

    def kv_copies(c, slot):
        m = ck * kvh
        return [pltpu.make_async_copy(w.at[pl.ds(pl.multiple_of(c * m, m), m)], kvb_s.at[slot, k], kvsem.at[slot, k])
                for k, w in enumerate((wk_hbm, wv_hbm))]

    def o_copies(c, slot):
        return [pltpu.make_async_copy(wo_hbm.at[pl.ds(pl.multiple_of(c * tile, tile), tile)], wo_s.at[slot], osem.at[slot])]

    def q_body(c, slot):
        def sub(s, _):
            m = 4 * blk
            rhs = jnp.concatenate(
                [qb_s[slot, pl.ds(pl.multiple_of(s * m + i * blk, blk), blk), :] for i in range(4)], axis=1)
            y = dot(pq_s[...], rhs)
            k0 = pl.multiple_of(c * cq + s * 4 * kq, 4 * kq)
            for h in range(heads):
                for p in range(2):
                    pair = [y[h * kq:(h + 1) * kq, (2 * p + e) * hd:(2 * p + e + 1) * hd] for e in range(2)]
                    w_s[pl.ds(k0 + 2 * kq * p, 2 * kq), h * hd:(h + 1) * hd] = jnp.concatenate(pair, axis=0).astype(BF16)
            return 0
        for s in range(cq // (4 * kq)):
            sub(s, 0)

    def kv_body(c, slot):
        def sub(s, _):
            m = 2 * blk
            rhs = jnp.concatenate(
                [kvb_s[slot, k, pl.ds(pl.multiple_of(s * m + i * blk, blk), blk), :] for k in range(2) for i in range(2)], axis=1)
            y = dot(pk_s[...], rhs)
            k0 = pl.multiple_of(c * ck + s * 2 * kk, 2 * kk)
            for k in range(2):
                for i in range(2):
                    for h in range(kvh):
                        col = heads * hd + (k * kvh + h) * hd
                        w_s[pl.ds(k0 + i * kk, kk), col:col + hd] = y[h * kk:(h + 1) * kk, (2 * k + i) * hd:(2 * k + i + 1) * hd].astype(BF16)
            return 0
        for s in range(ck // (2 * kk)):
            sub(s, 0)

    run_kv = ring(dm // ck, kvb_s.shape[0], kv_copies, kv_body)
    run_q = ring(dm // cq, qb_s.shape[0], q_copies, q_body)

    bar = pltpu.get_barrier_semaphore()
    for d in range(1, n):
        pl.semaphore_signal(bar, inc=1, device_id={"sp": lax.rem(me + d, n)}, device_id_type=MESH)
    own = pltpu.make_async_copy(x_hbm.at[pl.ds(me * nb, nb)], x_s.at[:, pl.ds(pl.multiple_of(me * tl, tl), tl), :], lsem)
    own.start()
    r_i = lax.broadcasted_iota(jnp.int32, (blk, blk), 0)
    c_i = lax.broadcasted_iota(jnp.int32, (blk, blk), 1)
    pq_s[...] = jnp.where(c_i == (r_i % kq) * heads + r_i // kq, 1.0, 0.0).astype(BF16)
    pk_s[...] = jnp.where(c_i == (r_i % kk) * kvh + r_i // kk, 1.0, 0.0).astype(BF16)
    pl.semaphore_wait(bar, n - 1)
    sends = []
    half = n // 2
    for d in [half] + [v for k in range(half - 1, 0, -1) for v in (k, n - k)]:
        peer = lax.rem(me + d, n)
        cp = pltpu.make_async_remote_copy(
            src_ref=x_hbm.at[pl.ds(peer * nb, nb)], dst_ref=x_s.at[:, pl.ds(pl.multiple_of(me * tl, tl), tl), :],
            send_sem=ssem.at[d], recv_sem=rsem.at[d], device_id={"sp": peer}, device_id_type=MESH)
        cp.start()
        sends.append(cp)

    run_kv()
    run_q()
    slots_o = wo_s.shape[0]
    n_o = wo_hbm.shape[0] // tile
    for c in range(slots_o):
        for cp in o_copies(c, c):
            cp.start()
    own.wait()
    for cp in sends:
        cp.wait()

    for b in range(nb):
        xb = x_s[b]
        a_s[b * seq:(b + 1) * seq, :] = rms_rows(xb, g_ref[...]).astype(BF16)
        acc_s[b * seq:(b + 1) * seq, :] = xb.astype(F32)

    def kv_proj(c, _):
        col = pl.multiple_of(heads * hd + c * tile, tile)
        val = dot(a_s[...], w_s[:, pl.ds(col, tile)]).astype(BF16)
        for h in range(grp):
            kv_s[c * grp + h] = val[:, h * hd:(h + 1) * hd]
        return 0
    lax.fori_loop(0, 2 * kvh // grp, kv_proj, 0, unroll=True)

    q_s[0] = dot(a_s[...], w_s[:, 0:tile]).astype(BF16)
    o_s[1] = jnp.zeros_like(o_s[1])
    row_t = lax.broadcasted_iota(jnp.int32, (grp * seq, seq), 0) % seq
    col_t = lax.broadcasted_iota(jnp.int32, (grp * seq, seq), 1)
    causal = row_t >= col_t

    def group(j, _):
        done = jnp.maximum(j - 1, 0)
        slot = lax.rem(done, slots_o)
        nxt = jnp.minimum(j + 1, n_o - 1)
        cur = lax.rem(j, 2)

        @pl.when(j != 1)
        def _():
            for cp in o_copies(done, slot):
                cp.wait()

        scores = []
        for b in range(nb):
            qb = q_s[cur, b * seq:(b + 1) * seq, :]
            q4 = jnp.concatenate([qb[:, g * hd:(g + 1) * hd] for g in range(grp)], axis=0)
            scores.append(dot_nt(q4, kv_s[j, b * seq:(b + 1) * seq, :]))
        q_next = dot(a_s[...], w_s[:, pl.ds(pl.multiple_of(nxt * tile, tile), tile)]).astype(BF16)
        probs = []
        for s in scores:
            s = jnp.where(causal, s * (hd ** -0.5), -jnp.inf)
            e = jnp.exp(s - jnp.max(s, axis=-1, keepdims=True))
            probs.append((e / jnp.sum(e, axis=-1, keepdims=True)).astype(BF16))
        acc_s[...] += dot(o_s[1 - cur], wo_s[slot])
        for b in range(nb):
            o = dot(probs[b], kv_s[kvh + j, b * seq:(b + 1) * seq, :]).astype(BF16)
            for g in range(grp):
                o_s[cur, b * seq:(b + 1) * seq, g * hd:(g + 1) * hd] = o[g * seq:(g + 1) * seq, :]
        q_s[1 - cur] = q_next

        @pl.when((j >= 1) & (j - 1 + slots_o < n_o))
        def _():
            for cp in o_copies(j - 1 + slots_o, slot):
                cp.start()
        return 0
    lax.fori_loop(0, n_o, group, 0)
    last = (n_o - 1) % slots_o
    for cp in o_copies(n_o - 1, last):
        cp.wait()
    h_ref[...] = (acc_s[...] + dot(o_s[(n_o - 1) % 2], wo_s[last])).astype(BF16)


def head(x, g, wq, wk, wv, wo, n):
    batch, tl, dm = x.shape
    heads, hd = wq.shape[1:]
    kvh = wk.shape[1]
    nb, seq = batch // n, tl * n
    rows = nb * seq
    grp = heads // kvh
    tile = grp * hd
    blk = 256
    cq, ck, slots_q, slots_o = 128, 320, 3, 3
    any_ = pl.BlockSpec(memory_space=pl.ANY)
    vm = pl.BlockSpec(memory_space=pltpu.VMEM)
    flat = lambda w: w.reshape(-1, w.shape[-1])
    return pl.pallas_call(
        functools.partial(head_kernel, n, heads, kvh, hd),
        out_shape=jax.ShapeDtypeStruct((rows, dm), BF16),
        in_specs=[any_, vm, any_, any_, any_, any_],
        out_specs=vm,
        scratch_shapes=[
            pltpu.VMEM((nb, seq, dm), BF16),
            pltpu.VMEM((dm, (heads + 2 * kvh) * hd), BF16),
            pltpu.VMEM((slots_q, cq * heads, hd), BF16),
            pltpu.VMEM((2, 2, ck * kvh, hd), BF16),
            pltpu.VMEM((slots_o, tile, dm), BF16),
            pltpu.VMEM((rows, dm), BF16),
            pltpu.VMEM((2 * kvh, rows, hd), BF16),
            pltpu.VMEM((2, rows, tile), BF16),
            pltpu.VMEM((2, rows, tile), BF16),
            pltpu.VMEM((rows, dm), F32),
            pltpu.VMEM((blk, blk), BF16),
            pltpu.VMEM((blk, blk), BF16),
            pltpu.SemaphoreType.DMA((n,)),
            pltpu.SemaphoreType.DMA((n,)),
            pltpu.SemaphoreType.DMA,
            pltpu.SemaphoreType.DMA((slots_q,)),
            pltpu.SemaphoreType.DMA((2, 2)),
            pltpu.SemaphoreType.DMA((slots_o,)),
        ],
        compiler_params=pltpu.CompilerParams(collective_id=0, has_side_effects=True, vmem_limit_bytes=63 << 20),
        name="head",
    )(x, g, flat(wq), flat(wk), flat(wv), flat(wo))


def zero_of(vals):
    return jnp.maximum(functools.reduce(jnp.minimum, vals, jnp.zeros_like(vals[0])), 0.0)


def tail_kernel(n, seq, dt_rank, n_state, h_ref, mg_ref, wg_hbm, wu_hbm, wd_hbm, ug_ref, wx_hbm, cw_ref, cb_ref, wxp_hbm,
                dtn_ref, bn_ref, cn_ref, wdt_hbm, dtb_ref, alog_ref, dsk_ref, wz_hbm, wo_hbm, o_hbm,
                w_s, d_s, u_s, acc_s, act_s, c_s, xi_s, r_s, dt_s, b_s, cc_s, dl_s, dx_s, y_s, a_s, st_s, z_s, gate_s, o_s,
                wxp_s, wdt_s, wsem, dsem, psem, ssem, rsem, lsem):
    me = lax.axis_index("sp")
    rows, dm = acc_s.shape
    slots, _, _, half_w = w_s.shape
    slots_d = d_s.shape[0]
    tile = 2 * half_w
    ne, nf = wx_hbm.shape[1] // tile, wg_hbm.shape[1] // half_w
    sub = tile // 128
    nb, tl = rows // seq, seq // n
    part = 256
    n_part = tile // part
    per = half_w // part
    tc = seq // n_part

    bar = pltpu.get_barrier_semaphore()
    for d in range(1, n):
        pl.semaphore_signal(bar, inc=1, device_id={"sp": lax.rem(me + d, n)}, device_id_type=MESH)

    def w_pair(k, a, b, ka, kb):
        slot = lax.rem(k, slots)
        return [pltpu.make_async_copy(w.at[:, pl.ds(pl.multiple_of(q * half_w, half_w), half_w)], w_s.at[slot, r], wsem.at[slot, r])
                for r, (w, q) in enumerate(((a, ka), (b, kb)))]

    def w_start(k):
        @pl.when(k < nf)
        def _():
            for cp in w_pair(k, wg_hbm, wu_hbm, k, k):
                cp.start()

        @pl.when((k >= nf) & (k < nf + ne))
        def _():
            for cp in w_pair(k, wx_hbm, wx_hbm, 2 * (k - nf), 2 * (k - nf) + 1):
                cp.start()

        @pl.when((k >= nf + ne) & (k < nf + 2 * ne))
        def _():
            for cp in w_pair(k, wz_hbm, wz_hbm, 2 * (k - nf - ne), 2 * (k - nf - ne) + 1):
                cp.start()

    def w_wait(k):
        for cp in w_pair(k, wg_hbm, wu_hbm, 0, 0):
            cp.wait()

    def d_copy(k, w, q):
        slot = lax.rem(k, slots_d)
        return pltpu.make_async_copy(w.at[pl.ds(pl.multiple_of(q * half_w, half_w), half_w)], d_s.at[slot], dsem.at[slot])

    def d_start(k):
        @pl.when(k < nf)
        def _():
            d_copy(k, wd_hbm, k).start()

        @pl.when((k >= nf) & (k < nf + 2 * ne))
        def _():
            d_copy(k, wo_hbm, k - nf).start()

    def d_wait(k):
        d_copy(k, wd_hbm, 0).wait()

    for k in range(max(slots, slots_d)):
        if k < slots:
            w_start(k)
        if k < slots_d:
            d_start(k)
    small = [pltpu.make_async_copy(wxp_hbm, wxp_s, psem.at[0]), pltpu.make_async_copy(wdt_hbm, wdt_s, psem.at[1])]
    for cp in small:
        cp.start()

    u_s[0:rows, :] = rms_rows(h_ref[...], mg_ref[...]).astype(BF16)
    acc_s[...] = h_ref[...].astype(F32)
    w_wait(0)
    act_s[0] = (silu(dot(u_s[0:rows, :], w_s[0, 0])) * dot(u_s[0:rows, :], w_s[0, 1])).astype(BF16)
    w_start(slots)

    def ff(k, _):
        slot, prev = lax.rem(k, slots), lax.rem(k - 1, slots_d)
        w_wait(k)
        d_wait(k - 1)
        gate = dot(u_s[0:rows, :], w_s[slot, 0])
        up = dot(u_s[0:rows, :], w_s[slot, 1])
        acc_s[...] += dot(act_s[lax.rem(k + 1, 2)], d_s[prev])
        act_s[lax.rem(k, 2)] = (silu(gate) * up).astype(BF16)
        w_start(k + slots)
        d_start(k - 1 + slots_d)
        return 0
    lax.fori_loop(1, nf, ff, 0)
    d_wait(nf - 1)
    h2 = (acc_s[...] + dot(act_s[(nf - 1) % 2], d_s[(nf - 1) % slots_d])).astype(BF16)
    d_start(nf - 1 + slots_d)
    acc_s[...] = h2.astype(F32)
    u_s[0:rows, :] = rms_rows(acc_s[...], ug_ref[...]).astype(BF16)

    r_s[...] = jnp.zeros_like(r_s)
    gate_s[...] = jnp.zeros_like(gate_s)

    def in_proj(e):
        k = nf + e
        slot = lax.rem(k, slots)
        w_wait(k)
        for r in range(2):
            xi_s[lax.rem(e, 2), :, r * half_w:(r + 1) * half_w] = dot(u_s[0:rows, :], w_s[slot, r]).astype(BF16)

    def conv(e):
        col = pl.ds(pl.multiple_of(e * tile, tile), tile)
        xi = xi_s[lax.rem(e, 2)].astype(F32)
        t_idx = lax.broadcasted_iota(jnp.int32, xi.shape, 0) % seq
        acc = cb_ref[col].astype(F32).reshape(1, -1) + xi * cw_ref[CONV - 1:CONV, col].astype(F32)
        for s in range(1, CONV):
            prev = jnp.where(t_idx >= s, pltpu.roll(xi, s, 0), 0.0)
            acc = acc + prev * cw_ref[CONV - 1 - s:CONV - s, col].astype(F32)
        c = silu(acc).astype(BF16)
        c_s[e] = c
        r_s[...] += dot_nt(c, wxp_s[:, col])

    in_proj(0)
    w_start(nf + slots)
    for cp in small:
        cp.wait()

    def phase_a(e, _):
        in_proj(e)
        conv(e - 1)
        w_start(nf + e + slots)
        return 0
    lax.fori_loop(1, ne, phase_a, 0)

    kz = nf + ne
    w_wait(kz)
    for r in range(2):
        z_s[0, :, r * half_w:(r + 1) * half_w] = dot(u_s[0:rows, :], w_s[kz % slots, r]).astype(BF16)
    conv(ne - 1)
    w_start(kz + slots)

    r = r_s[...]
    dt_s[...] = rms_rows(r[:, :dt_rank], dtn_ref[...]).astype(BF16)
    bm = rms_rows(r[:, dt_rank:dt_rank + n_state], bn_ref[...])
    cm = rms_rows(r[:, dt_rank + n_state:], cn_ref[...])
    for k in range(n_state):
        b_s[k] = jnp.broadcast_to(bm[:, k:k + 1], (rows, 128))
        cc_s[k] = jnp.broadcast_to(cm[:, k:k + 1], (rows, 128))

    def phase_b(e, _):
        col = pl.ds(pl.multiple_of(e * tile, tile), tile)
        zc, zn = lax.rem(e, 2), lax.rem(e + 1, 2)
        z_tile, o_tile = jnp.minimum(e + 1, ne - 1), jnp.maximum(e - 1, 0)
        slot_z = lax.rem(kz + z_tile, slots)

        @pl.when(e + 1 < ne)
        def _():
            w_wait(kz + e + 1)

        @pl.when(e != 1)
        def _():
            for q in range(2):
                d_wait(nf + 2 * o_tile + q)

        delta = softplus(dot(dt_s[...], wdt_s[:, col]) + dtb_ref[:, col])
        dx = delta * c_s[e].astype(F32)
        a2 = -jnp.exp(alog_ref[:, col]) * LOG2E
        for j in range(sub):
            dl_s[pl.ds(j, rows, stride=sub), :] = delta[:, j * 128:(j + 1) * 128]
            dx_s[pl.ds(j, rows, stride=sub), :] = dx[:, j * 128:(j + 1) * 128]
            a_s[pl.ds(j, n_state, stride=sub), :] = a2[:, j * 128:(j + 1) * 128]
        st_s[...] = jnp.zeros_like(st_s)

        def chunk(c, _):
            spare = pl.multiple_of(rows + 16 * lax.div(c, n_part), 16)
            k0 = pl.multiple_of(c * part, part)
            kp = pl.multiple_of(lax.rem(c, per) * part, part)
            slot_o = lax.rem(nf + 2 * o_tile + c // per, slots_d)
            n_k = dm // 256
            places = [(p * (nb * tc - LAG)) // (2 * n_k) for p in range(2 * n_k)]
            lhs, after = [], {}

            def fence(ref, y):
                ref[pl.ds(spare, 16), 0:128] = jnp.concatenate([y, y], axis=0).astype(BF16)

            for b in range(nb):
                state = [st_s[b * n_state + k] for k in range(n_state)]
                for tt in range(tc):
                    step = b * tc + tt
                    tok = b * seq + c * tc + tt
                    row = pl.multiple_of(tok * sub, sub)
                    dl = dl_s[pl.ds(row, sub), :]
                    dxt = dx_s[pl.ds(row, sub), :]
                    if step in after:
                        dl = dl + after[step]
                    parts = [None] * 2
                    for k in range(n_state):
                        bb = b_s[k, pl.ds(tok, sub, stride=0), :]
                        ct = cc_s[k, pl.ds(tok, sub, stride=0), :]
                        s = jnp.exp2(dl * a_s[k * sub:(k + 1) * sub, :]) * state[k] + dxt * bb
                        state[k] = s
                        term = s * ct
                        parts[k % 2] = term if parts[k % 2] is None else parts[k % 2] + term
                    y = parts[0] + parts[1]
                    y_s[pl.ds(row, sub), :] = y
                    if step == tc - 1:
                        after[tc] = zero_of([y])
                    if step in places:
                        p = places.index(step)
                        q = p // 2
                        if p % 2 == 0:
                            fence(u_s, y)
                            lhs.append(u_s[0:rows, q * 256:(q + 1) * 256])
                        else:
                            fence(gate_s, y)
                            lanes = slice(q * 256, (q + 1) * 256)
                            ov = dot(gate_s[0:rows, pl.ds(k0, part)], d_s[slot_o, pl.ds(kp, part), lanes])
                            acc_s[:, lanes] += ov
                            after[step + LAG] = zero_of([ov[rows - 8:, l0:l0 + 128] for l0 in (0, 128)])
                        if p == 2 * n_k - 2:
                            zv = dot(jnp.concatenate(lhs, axis=1), w_s[slot_z, c // per, :, pl.ds(kp, part)])
                            z_s[zn, :, pl.ds(k0, part)] = zv.astype(BF16)
                            after[step + LAG] = zero_of([zv[r0:r0 + 8, l0:l0 + 128] for r0 in (0, rows - 8) for l0 in (0, part - 128)])
                for k in range(n_state):
                    st_s[b * n_state + k] = state[k]
            return 0

        lax.fori_loop(0, n_part, chunk, 0)
        w_start(kz + e + 1 + slots)

        @pl.when(e >= 1)
        def _():
            for q in range(2):
                d_start(nf + 2 * (e - 1) + q + slots_d)

        for j in range(sub):
            lanes = slice(j * 128, (j + 1) * 128)
            dlanes = pl.ds(pl.multiple_of(e * tile + j * 128, 128), 128)
            y = y_s[pl.ds(j, rows, stride=sub), :] + dsk_ref[:, dlanes] * c_s[e, :, lanes].astype(F32)
            gate_s[0:rows, lanes] = (y * silu(z_s[zc, :, lanes].astype(F32))).astype(BF16)
        return 0
    lax.fori_loop(0, ne, phase_b, 0)

    n_out, _, _, w = o_s.shape
    pl.semaphore_wait(bar, n - 1)
    half = n // 2
    order = [half] + [v for k in range(half - 1, 0, -1) for v in (k, n - k)]
    copies = []

    def send(q):
        lanes = slice(q * w, (q + 1) * w)
        for d in order:
            peer = lax.rem(me + d, n)
            cp = pltpu.make_async_remote_copy(
                src_ref=o_s.at[q, :, pl.ds(pl.multiple_of(peer * tl, tl), tl), :],
                dst_ref=o_hbm.at[pl.ds(me * nb, nb), :, lanes],
                send_sem=ssem.at[q, d], recv_sem=rsem.at[q, d], device_id={"sp": peer}, device_id_type=MESH)
            cp.start()
            copies.append(cp)
        cp = pltpu.make_async_copy(o_s.at[q, :, pl.ds(pl.multiple_of(me * tl, tl), tl), :],
                                   o_hbm.at[pl.ds(me * nb, nb), :, lanes], lsem.at[q])
        cp.start()
        copies.append(cp)

    for q in range(2):
        d_wait(nf + 2 * (ne - 1) + q)
    s0, s1 = [(nf + 2 * (ne - 1) + q) % slots_d for q in range(2)]
    for q in range(n_out):
        lanes = slice(q * w, (q + 1) * w)
        val = acc_s[:, lanes] + dot(gate_s[0:rows, :half_w], d_s[s0, :, lanes]) + dot(gate_s[0:rows, half_w:], d_s[s1, :, lanes])
        for b in range(nb):
            o_s[q, b] = val[b * seq:(b + 1) * seq, :].astype(BF16)
        if q:
            send(q - 1)
    send(n_out - 1)
    for cp in copies:
        cp.wait()


def tail(h, mg, wg, wu, wd, ug, wx, wz, cw, cb, wxp_t, dtn, bn, cn, wdt, dtb, alog_t, dsk, wo, seq, n, half_w=512, n_out=10, slots=3, slots_d=4):
    rows, dm = h.shape
    inner = wx.shape[1]
    dt_rank, n_state = wdt.shape[0], alog_t.shape[0]
    nr = wxp_t.shape[0]
    tile = 2 * half_w
    ne = inner // tile
    sub = tile // 128
    nb, tl = rows // seq, seq // n
    any_ = pl.BlockSpec(memory_space=pl.ANY)
    vm = pl.BlockSpec(memory_space=pltpu.VMEM)
    return pl.pallas_call(
        functools.partial(tail_kernel, n, seq, dt_rank, n_state),
        out_shape=jax.ShapeDtypeStruct((nb * n, tl, dm), BF16),
        in_specs=[vm, vm, any_, any_, any_, vm, any_, vm, vm, any_, vm, vm, vm, any_, vm, vm, vm, any_, any_],
        out_specs=any_,
        scratch_shapes=[
            pltpu.VMEM((slots, 2, dm, half_w), BF16),
            pltpu.VMEM((slots_d, half_w, dm), BF16),
            pltpu.VMEM((rows + 16, dm), BF16),
            pltpu.VMEM((rows, dm), F32),
            pltpu.VMEM((2, rows, half_w), BF16),
            pltpu.VMEM((ne, rows, tile), BF16),
            pltpu.VMEM((2, rows, tile), BF16),
            pltpu.VMEM((rows, nr), F32),
            pltpu.VMEM((rows, dt_rank), BF16),
            pltpu.VMEM((n_state, rows, 128), F32),
            pltpu.VMEM((n_state, rows, 128), F32),
            pltpu.VMEM((rows * sub, 128), F32),
            pltpu.VMEM((rows * sub, 128), F32),
            pltpu.VMEM((rows * sub, 128), F32),
            pltpu.VMEM((n_state * sub, 128), F32),
            pltpu.VMEM((nb * n_state, sub, 128), F32),
            pltpu.VMEM((2, rows, tile), BF16),
            pltpu.VMEM((rows + 16, tile), BF16),
            pltpu.VMEM((n_out, nb, seq, dm // n_out), BF16),
            pltpu.VMEM((nr, inner), BF16),
            pltpu.VMEM((dt_rank, inner), BF16),
            pltpu.SemaphoreType.DMA((slots, 2)),
            pltpu.SemaphoreType.DMA((slots_d,)),
            pltpu.SemaphoreType.DMA((2,)),
            pltpu.SemaphoreType.DMA((n_out, n)),
            pltpu.SemaphoreType.DMA((n_out, n)),
            pltpu.SemaphoreType.DMA((n_out,)),
        ],
        compiler_params=pltpu.CompilerParams(collective_id=1, has_side_effects=True, vmem_limit_bytes=55 << 20),
        name="tail",
    )(h, mg, wg, wu, wd, ug, wx, cw, cb, wxp_t, dtn, bn, cn, wdt, dtb, alog_t, dsk, wz, wo)


def layer_pair(hidden, attn_norm, w_q, w_k, w_v, w_o, mlp_norm, w_gate, w_up, w_down, mamba_norm, w_in_x, w_in_z, conv_w, conv_b, w_xproj, dt_norm, b_norm, c_norm, w_dt, dt_bias, a_log, d_skip, w_out, n_shards):
    batch, tl, dm = hidden.shape
    seq = tl * n_shards
    row = lambda v: v.reshape(1, -1)
    h = head(hidden, attn_norm, w_q, w_k, w_v, w_o, n_shards)
    return tail(h, mlp_norm, w_gate, w_up, w_down, mamba_norm, w_in_x, w_in_z, conv_w, conv_b, w_xproj.T, row(dt_norm), row(b_norm), row(c_norm), w_dt, row(dt_bias), a_log.T, row(d_skip), w_out, seq, n_shards)


def solution(mesh):
    act_spec = P("dp", "sp", None)
    return jax.shard_map(
        functools.partial(layer_pair, n_shards=mesh.shape["sp"]),
        mesh=mesh,
        in_specs=(act_spec,) + (P(),) * 23,
        out_specs=act_spec,
        check_vma=False,
    )
```
